32 devices in a mesh: dp: 2 (over x), tp: 4 (over z), ep: 4 (over y, core).
Axes of the slice: x: 2, y: 2, z: 4, core: 2. Of those that a mesh axis runs over, the one named last changes fastest.
Arguments:
- tokens: bfloat16 [2048, 768], P(('dp', 'ep')), parts along dimension 0
- grad_out: bfloat16 [2048, 768], P(('dp', 'ep')), parts along dimension 0
- w_router: bfloat16 [768, 16], replicated
- w_in: bfloat16 [16, 768, 3072], P('ep', None, 'tp')
- w_out: bfloat16 [16, 3072, 768], P('ep', 'tp')
- expert_ids: int32 [2048], P(('dp', 'ep')), parts along dimension 0
Outputs:
- output 1: bfloat16 [2048, 768], P(('dp', 'ep')), parts along dimension 0
- output 2: bfloat16 [2048, 768], P(('dp', 'ep')), parts along dimension 0
- output 3: float32 [32, 768, 3072], P(('dp', 'ep'), None, 'tp'), parts along dimension 0
- output 4: float32 [32, 3072, 768], P(('dp', 'ep'), 'tp'), parts along dimension 0
- output 5: float32 [1536, 16], P('dp'), parts along dimension 0
There are 2 independent parts. The reference program is written for one: setup_inputs(seed, part) draws one part's arguments, and reference() takes and returns one part's arrays. A program takes and returns all parts, laid end to end along the dimension named above; an argument that names none is the same for every part.
All inputs are finite; a program needn't handle non-finite values.
Results may differ from the reference program's by a relative error of at most 0.00644388.
Values are sent between devices in bfloat16 or wider.
A program may use at most 1 GiB of HBM per device.

```python
import jax
import jax.numpy as jnp
from jax import lax

D_MODEL = 768
D_FF = 3072
EXPERTS = 16
TOKENS_DEV = 256
EP_RANKS = 4

CAPACITY = (6 * TOKENS_DEV + 5 * EXPERTS - 1) // (5 * EXPERTS)
N_TOKENS = EP_RANKS * TOKENS_DEV
N_SLOTS = EXPERTS * CAPACITY


def draw_routes(route_key):
    key_hot, key_order, key_rest = jax.random.split(route_key, 3)
    hot_expert = jax.random.randint(key_hot, (EP_RANKS, 1), 0, EXPERTS)
    rest_ids = jax.random.randint(key_rest, (EP_RANKS, TOKENS_DEV), 0, EXPERTS)
    order_keys = jax.random.split(key_order, EP_RANKS)
    rank_of = jax.vmap(lambda one_key: jax.random.permutation(one_key, TOKENS_DEV))(order_keys)
    hot_count = CAPACITY + CAPACITY // 2 + 1
    cover_ids = (rank_of - hot_count) % EXPERTS
    route_ids = jnp.where(rank_of < hot_count, hot_expert, jnp.where(rank_of < hot_count + EXPERTS, cover_ids, rest_ids))
    return route_ids.reshape(N_TOKENS).astype(jnp.int32)


def setup_inputs(seed: int = 0, part: int = 0) -> dict:
    part_key = jax.random.fold_in(jax.random.key(seed), part)
    rand_keys = jax.random.split(part_key, 3)
    weight_keys = jax.random.split(jax.random.key(seed + 1), 3)
    tokens = jax.random.normal(rand_keys[0], (N_TOKENS, D_MODEL), jnp.float32)
    grad_out = jax.random.normal(rand_keys[1], (N_TOKENS, D_MODEL), jnp.float32)
    w_router = jax.random.normal(weight_keys[0], (D_MODEL, EXPERTS), jnp.float32) * D_MODEL ** -0.5
    w_in = jax.random.normal(weight_keys[1], (EXPERTS, D_MODEL, D_FF), jnp.float32) * D_MODEL ** -0.5
    w_out = jax.random.normal(weight_keys[2], (EXPERTS, D_FF, D_MODEL), jnp.float32) * D_FF ** -0.5
    return {
        "tokens": tokens.astype(jnp.bfloat16),
        "grad_out": grad_out.astype(jnp.bfloat16),
        "w_router": w_router.astype(jnp.bfloat16),
        "w_in": w_in.astype(jnp.bfloat16),
        "w_out": w_out.astype(jnp.bfloat16),
        "expert_ids": draw_routes(rand_keys[2]),
    }


def dispatch(rows, slot_index):
    slot_buf = jnp.zeros((N_SLOTS + 1, D_MODEL), rows.dtype).at[slot_index].set(rows)
    return slot_buf[:N_SLOTS]


def combine(slot_buf, slot_index):
    padded = jnp.concatenate([slot_buf, jnp.zeros((1, D_MODEL), slot_buf.dtype)], axis=0)
    return jnp.take(padded, slot_index, axis=0)


def by_expert(source_bufs):
    return source_bufs.reshape(EP_RANKS, EXPERTS, CAPACITY, D_MODEL).transpose(1, 0, 2, 3).reshape(EXPERTS, EP_RANKS * CAPACITY, D_MODEL)


def by_source(expert_bufs):
    return expert_bufs.reshape(EXPERTS, EP_RANKS, CAPACITY, D_MODEL).transpose(1, 0, 2, 3).reshape(EP_RANKS, N_SLOTS, D_MODEL)


def expert_step(operands):
    slot_rows, dy_rows, w_in_e, w_out_e = operands
    pre_act = jnp.dot(slot_rows, w_in_e, preferred_element_type=jnp.float32)
    act_val, act_vjp = jax.vjp(jax.nn.gelu, pre_act)
    hidden = act_val.astype(jnp.bfloat16)
    y_rows = jnp.dot(hidden, w_out_e, preferred_element_type=jnp.float32).astype(jnp.bfloat16)
    d_hidden = jnp.dot(dy_rows, w_out_e.T, preferred_element_type=jnp.float32)
    d_pre = act_vjp(d_hidden)[0].astype(jnp.bfloat16)
    grad_out_e = jnp.dot(hidden.T, dy_rows, preferred_element_type=jnp.float32)
    grad_in_e = jnp.dot(slot_rows.T, d_pre, preferred_element_type=jnp.float32)
    d_slot = jnp.dot(d_pre, w_in_e.T, preferred_element_type=jnp.float32).astype(jnp.bfloat16)
    return y_rows, d_slot, grad_in_e, grad_out_e


def reference(tokens, grad_out, w_router, w_in, w_out, expert_ids):
    route_ids = expert_ids.reshape(EP_RANKS, TOKENS_DEV)
    one_hot = (route_ids[:, :, None] == jnp.arange(EXPERTS)[None, None, :]).astype(jnp.int32)
    position = jnp.sum(jnp.cumsum(one_hot, axis=1) * one_hot, axis=2) - 1
    slot_index = jnp.where(position < CAPACITY, route_ids * CAPACITY + position, N_SLOTS)
    chosen = expert_ids[:, None] == jnp.arange(EXPERTS)[None, :]
    logits = jnp.dot(tokens, w_router, preferred_element_type=jnp.float32)
    router_prob = jax.nn.softmax(logits, axis=-1)
    gate_prob = jnp.sum(jnp.where(chosen, router_prob, 0.0), axis=1)
    dy_tok = (gate_prob[:, None] * grad_out.astype(jnp.float32)).astype(jnp.bfloat16)
    slot_rows = jax.vmap(dispatch)(tokens.reshape(EP_RANKS, TOKENS_DEV, D_MODEL), slot_index)
    dy_rows = jax.vmap(dispatch)(dy_tok.reshape(EP_RANKS, TOKENS_DEV, D_MODEL), slot_index)
    y_rows, d_slot, grad_w_in, grad_w_out = lax.map(expert_step, (by_expert(slot_rows), by_expert(dy_rows), w_in, w_out))
    y_tok = jax.vmap(combine)(by_source(y_rows), slot_index).reshape(N_TOKENS, D_MODEL)
    dx_moe = jax.vmap(combine)(by_source(d_slot), slot_index).reshape(N_TOKENS, D_MODEL)
    moe_out = (gate_prob[:, None] * y_tok.astype(jnp.float32)).astype(jnp.bfloat16)
    d_gate = jnp.sum(grad_out.astype(jnp.float32) * y_tok.astype(jnp.float32), axis=1)
    d_logits = (d_gate[:, None] * router_prob * (chosen.astype(jnp.float32) - gate_prob[:, None])).astype(jnp.bfloat16)
    router_grad = jnp.dot(d_logits, w_router.T, preferred_element_type=jnp.float32)
    grad_tokens = (dx_moe.astype(jnp.float32) + router_grad).astype(jnp.bfloat16)
    grad_w_router = jnp.dot(tokens.T, d_logits, preferred_element_type=jnp.float32)
    return moe_out, grad_tokens, grad_w_in, grad_w_out, grad_w_router
```

```python
import functools

import jax
import jax.numpy as jnp
from jax import lax
from jax.experimental import pallas as pl
from jax.experimental.pallas import tpu as pltpu
from jax.sharding import PartitionSpec as P

MESH = pl.DeviceIdType.MESH
F32, BF16 = jnp.float32, jnp.bfloat16
GELU_C = 0.7978845608028654
GELU_K = 0.044715
N_EP, N_TP, N_PAIR = 4, 4, 2


def dot(a, b, dims=((1,), (0,))):
    return lax.dot_general(a, b, (dims, ((), ())), preferred_element_type=F32)


def pair_masks(rows, block, cap):
    row = lax.broadcasted_iota(jnp.int32, (rows, 1), 0)
    first = lax.rem(row, block) < cap
    return jnp.where(first, 1.0, 0.0).astype(BF16), jnp.where(first, 0.0, 1.0).astype(BF16)


def moe_kernel(
    cap,
    ids_ref, wg_ref, x_hbm, gy_hbm, wi_hbm, wo_hbm,
    out_hbm, dx_hbm, dwg_hbm, h_hbm, da_hbm, xr_hbm, dyr_hbm,
    x_v, gy_v, wi_v, wo_v,
    onehot_slots, router_v, send_v, recv_v, act_v, h_v, da_v,
    part_v, relay_in, relay_out, fin_in, red_v, slots_v,
    out_v, dx_v, dwg_part, dwg_in, dwg_v,
    load_sem, store_sem, disp_send, disp_recv, rs_send, rs_recv, hop_send, hop_recv, ag_send, ag_recv, wg_send, wg_recv,
):
    block = 2 * cap
    rows = N_EP * block
    n_tok, d_model = x_v.shape
    n_exp = wg_ref.shape[1]
    half = d_model // 2
    z, j = lax.axis_index("tp"), lax.axis_index("ep")
    right, left, far = lax.rem(z + 1, N_TP), lax.rem(z + 3, N_TP), lax.rem(z + 2, N_TP)
    ep_peer = [lax.rem(j + k, N_EP) for k in range(N_EP)]

    def remote(src, dst, ssem, rsem, **dev):
        return pltpu.make_async_remote_copy(
            src_ref=src, dst_ref=dst, send_sem=ssem, recv_sem=rsem, device_id=dev, device_id_type=MESH
        )

    load_x = pltpu.make_async_copy(x_hbm, x_v, load_sem.at[0])
    load_gy = pltpu.make_async_copy(gy_hbm, gy_v, load_sem.at[1])
    load_wi = [pltpu.make_async_copy(wi_hbm.at[pl.ds(2 * p, 2)], wi_v.at[pl.ds(2 * p, 2)], load_sem.at[2 + p]) for p in range(2)]
    load_wo = [pltpu.make_async_copy(wo_hbm.at[pl.ds(2 * p, 2)], wo_v.at[pl.ds(2 * p, 2)], load_sem.at[4 + p]) for p in range(2)]
    load_x.start()
    load_gy.start()
    for p in range(2):
        load_wi[p].start()
        load_wo[p].start()

    barrier = pltpu.get_barrier_semaphore()
    for dev in [{"tp": right}, {"tp": left}] + [{"ep": ep_peer[k]} for k in range(1, N_EP)]:
        pl.semaphore_signal(barrier, inc=1, device_id=dev, device_id_type=MESH)

    ids = ids_ref[...]
    chosen = ids == lax.broadcasted_iota(jnp.int32, (n_exp, n_tok), 0)
    onehot = jnp.where(chosen, 1.0, 0.0)
    before = lax.broadcasted_iota(jnp.int32, (n_tok, n_tok), 0) < lax.broadcasted_iota(jnp.int32, (n_tok, n_tok), 1)
    counts = dot(onehot.astype(BF16), jnp.where(before, 1.0, 0.0).astype(BF16))
    pos = jnp.sum(counts * onehot, axis=0, keepdims=True)
    base = ((ids >> 1) & 1) * rows + (ids >> 2) * block + (ids & 1) * cap
    slot = jnp.where(pos < cap, base.astype(F32) + pos, -1.0)
    slot_iota = lax.broadcasted_iota(jnp.int32, (2 * rows, n_tok), 0).astype(F32)
    onehot_slots[...] = jnp.where(slot_iota == slot, 1.0, 0.0).astype(BF16)

    pl.semaphore_wait(barrier, 5)

    def dispatch(t, tok_rows):
        packed = dot(onehot_slots[...], tok_rows).astype(BF16)
        send_v[t] = packed.reshape(2, N_EP, block, d_model)

    def disp_copy(t, p, k):
        return remote(
            send_v.at[t, p, ep_peer[k]], recv_v.at[t, p, j], disp_send.at[t, p, k - 1], disp_recv.at[t, p, k - 1], ep=ep_peer[k]
        )

    def start_dispatch(t):
        for p in range(N_PAIR):
            for k in (2, 1, 3):
                disp_copy(t, p, k).start()
        for p in range(N_PAIR):
            recv_v[t, p, j] = send_v[t, p, j]

    load_x.wait()
    dispatch(0, x_v[...])
    start_dispatch(0)

    logits = dot(wg_ref[...], x_v[...], ((0,), (1,)))
    expd = jnp.exp(logits - jnp.max(logits, axis=0, keepdims=True))
    prob = expd / jnp.sum(expd, axis=0, keepdims=True)
    gate_row = jnp.sum(jnp.where(chosen, prob, 0.0), axis=0, keepdims=True)
    router_v[...] = prob * (onehot - gate_row)
    gate_col = jnp.transpose(jnp.broadcast_to(gate_row, (128, n_tok)))
    gate_v = gate_col[:, :1]
    load_gy.wait()
    dispatch(1, (gate_v * gy_v[...].astype(F32)).astype(BF16))
    start_dispatch(1)

    mask0, mask1 = pair_masks(rows, block, cap)

    def wait_rows(t, p):
        for k in range(1, N_EP):
            disp_copy(t, p, k).wait_recv()
        return recv_v[t, p].reshape(rows, d_model)

    def pair_dot(lhs, w_ref, p, dims=((1,), (0,))):
        return dot(lhs * mask0, w_ref[2 * p], dims) + dot(lhs * mask1, w_ref[2 * p + 1], dims)

    def blk(zz, p):
        return lax.rem(zz + 2 * p, N_TP)

    def rs_copy(i, p, d, m):
        nxt = right if d == 0 else left
        sem = (rs_send.at[i, d, m], rs_recv.at[i, d, m])
        if m == 0:
            return remote(part_v.at[i, d, blk(far, p)], relay_in.at[i, d], *sem, tp=nxt)
        if m == 1:
            return remote(part_v.at[i, 1 - d, blk(nxt, p)], fin_in.at[i, d, 1 - d], *sem, tp=nxt)
        return remote(relay_out.at[i, d], fin_in.at[i, d, d], *sem, tp=nxt)

    def rs_start(t, p, part):
        i = 2 * t + p
        part_v[i, 0] = part[:, :half].reshape(N_EP, block, half)
        part_v[i, 1] = part[:, half:].reshape(N_EP, block, half)
        for m in (0, 1):
            for d in (0, 1):
                rs_copy(i, p, d, m).start()

    def rs_relay(t, p):
        i = 2 * t + p
        for d in (0, 1):
            rs_copy(i, p, d, 0).wait_recv()
            relay_out[i, d] = relay_in[i, d] + part_v[i, d, blk(right if d == 0 else left, p)]
            rs_copy(i, p, d, 2).start()

    def hop_copy(i, p, k):
        return remote(red_v.at[i], slots_v.at[i, j], hop_send.at[i], hop_recv.at[i, k - 1], ep=ep_peer[k])

    def rs_final(t, p):
        i = 2 * t + p
        for d in (0, 1):
            rs_copy(i, p, d, 1).wait_recv()
            rs_copy(i, p, d, 2).wait_recv()
        mine = blk(z, p)
        whole = [part_v[i, h, mine] + fin_in[i, 0, h] + fin_in[i, 1, h] for h in (0, 1)]
        red_v[i] = jnp.concatenate(whole, axis=1).astype(BF16)
        for k in range(1, N_EP):
            @pl.when(mine == ep_peer[k])
            def _():
                hop_copy(i, p, k).start()

        @pl.when(mine == j)
        def _():
            slots_v[i, j] = red_v[i]

    def ag_copy(i, hlf, n, dev):
        part = slots_v.at[i, pl.ds(2 * hlf, 2)]
        return remote(part, part, ag_send.at[i, n], ag_recv.at[i, hlf], tp=dev)

    def place(p):
        return lax.rem(z + N_TP - blk(j, p) + 0, N_TP)

    def ag_root(t, p):
        i = 2 * t + p

        @pl.when(place(p) == 0)
        def _():
            for k in range(1, N_EP):
                hop_copy(i, p, k).wait_recv()
            ag_copy(i, 0, 0, right).start()
            ag_copy(i, 1, 1, left).start()
            ag_copy(i, 1, 2, right).start()
            ag_copy(i, 0, 3, left).start()

    def ag_forward(t, p):
        i = 2 * t + p

        @pl.when(place(p) == 1)
        def _():
            ag_copy(i, 0, 0, right).wait_recv()
            ag_copy(i, 0, 0, right).start()

        @pl.when(place(p) == 3)
        def _():
            ag_copy(i, 1, 0, left).wait_recv()
            ag_copy(i, 1, 0, left).start()

    def ag_wait(t, p):
        i = 2 * t + p

        @pl.when((place(p) == 1) | (place(p) == 2))
        def _():
            ag_copy(i, 1, 0, right).wait_recv()

        @pl.when((place(p) == 3) | (place(p) == 2))
        def _():
            ag_copy(i, 0, 0, right).wait_recv()

    def forward(p):
        load_wi[p].wait()
        xr = wait_rows(0, p)
        a = pair_dot(xr, wi_v, p)
        act_v[p] = a
        h = (0.5 * a * (1.0 + jnp.tanh(GELU_C * (a + GELU_K * a * a * a)))).astype(BF16)
        h_v[p] = h
        load_wo[p].wait()
        rs_start(0, p, pair_dot(h, wo_v, p))

    def backward(p):
        dyr = wait_rows(1, p)
        dh = pair_dot(dyr, wo_v, p, ((1,), (1,)))
        a = act_v[p]
        a2 = a * a
        th = jnp.tanh(GELU_C * (a + GELU_K * a2 * a))
        slope = 0.5 * (1.0 + th) + 0.5 * a * (1.0 - th * th) * (GELU_C * (1.0 + 3.0 * GELU_K * a2))
        da = (dh * slope).astype(BF16)
        da_v[p] = da
        rs_start(1, p, pair_dot(da, wi_v, p, ((1,), (1,))))

    def combine(t):
        both = jnp.concatenate([slots_v[2 * t + p].reshape(rows, d_model) for p in range(2)], axis=0)
        return dot(onehot_slots[...], both, ((0,), (0,)))

    stores = []

    def store(src, dst):
        cp = pltpu.make_async_copy(src, dst, store_sem.at[len(stores)])
        cp.start()
        stores.append(cp)

    forward(0)
    forward(1)
    rs_relay(0, 0)
    backward(0)
    rs_relay(0, 1)
    rs_final(0, 0)
    backward(1)
    store(h_v, h_hbm)
    store(da_v, da_hbm)
    store(recv_v.at[0], xr_hbm)
    store(recv_v.at[1], dyr_hbm)
    rs_final(0, 1)
    ag_root(0, 0)
    rs_relay(1, 0)
    ag_root(0, 1)
    ag_forward(0, 0)
    rs_relay(1, 1)
    ag_forward(0, 1)
    rs_final(1, 0)
    rs_final(1, 1)
    ag_wait(0, 0)
    ag_wait(0, 1)
    ag_root(1, 0)
    ag_root(1, 1)

    y_tok = combine(0)
    out_v[...] = (gate_v * y_tok).astype(BF16)
    store(out_v, out_hbm)
    d_gate = jnp.sum(gy_v[...].astype(F32) * y_tok, axis=1, keepdims=True)
    d_gate_row = jnp.transpose(jnp.broadcast_to(d_gate, (n_tok, 128)))[:1]
    d_logits = d_gate_row * router_v[...]
    dwg_part[...] = dot(d_logits.astype(BF16), x_v[...])

    def wg_copy(k):
        return remote(dwg_part, dwg_in.at[k - 1], wg_send.at[k - 1], wg_recv.at[k - 1], ep=ep_peer[k])

    for k in range(1, N_EP):
        wg_copy(k).start()
    ag_forward(1, 0)
    router_grad = dot(jnp.transpose(d_logits).astype(BF16), wg_ref[...], ((1,), (1,)))
    ag_forward(1, 1)
    for k in range(1, N_EP):
        wg_copy(k).wait_recv()
    dwg_v[...] = (dwg_part[...] + dwg_in[1]) + (dwg_in[0] + dwg_in[2])
    store(dwg_v, dwg_hbm)
    ag_wait(1, 0)
    ag_wait(1, 1)
    dx_v[...] = (combine(1) + router_grad).astype(BF16)
    store(dx_v, dx_hbm)

    for t in range(2):
        for p in range(N_PAIR):
            i = 2 * t + p
            for k in range(1, N_EP):
                disp_copy(t, p, k).wait_send()
            for d in (0, 1):
                for m in range(3):
                    rs_copy(i, p, d, m).wait_send()

            @pl.when(blk(z, p) != j)
            def _():
                hop_copy(i, p, 1).wait_send()

            @pl.when(place(p) == 0)
            def _():
                for n, hlf in enumerate((0, 1, 1, 0)):
                    ag_copy(i, hlf, n, right).wait_send()

            @pl.when((place(p) == 1) | (place(p) == 3))
            def _():
                ag_copy(i, 0, 0, right).wait_send()
    for k in range(1, N_EP):
        wg_copy(k).wait_send()
    for cp in stores:
        cp.wait()


def grads_kernel(
    cap, h_ref, da_ref, xr_ref, dyr_ref, out_ref, dx_ref, dwg_ref,
    o_out, o_dx, o_wi, o_wo, o_dwg, stage, sem,
):
    block = 2 * cap
    rows = N_EP * block
    d_model = xr_ref.shape[-1]
    o_out[...] = out_ref[...]
    o_dx[...] = dx_ref[...]
    o_dwg[...] = jnp.transpose(dwg_ref[...])
    masks = pair_masks(rows, block, cap)
    copies = []
    for e in range(4):
        p, m = e // 2, masks[e % 2]
        xr = xr_ref[p].reshape(rows, d_model)
        dyr = dyr_ref[p].reshape(rows, d_model)
        stage[2 * e] = dot(h_ref[p] * m, dyr, ((0,), (0,)))
        copies.append(pltpu.make_async_copy(stage.at[2 * e], o_wo.at[e], sem.at[2 * e]))
        copies[-1].start()
        stage[2 * e + 1] = dot(xr * m, da_ref[p], ((0,), (0,)))
        copies.append(pltpu.make_async_copy(stage.at[2 * e + 1], o_wi.at[e], sem.at[2 * e + 1]))
        copies[-1].start()
    for cp in copies:
        cp.wait()


def solution(mesh):
    row_spec = P(("dp", "ep"), None)

    def local_block(tokens, grad_out, w_router, w_in, w_out, expert_ids):
        n_tok, d_model = tokens.shape
        n_exp = w_router.shape[1]
        n_loc, _, f_loc = w_in.shape
        cap = (6 * n_tok + 5 * n_exp - 1) // (5 * n_exp)
        block, rows, half = 2 * cap, 8 * cap, d_model // 2
        S = jax.ShapeDtypeStruct
        any_spec, vmem_spec = pl.BlockSpec(memory_space=pl.ANY), pl.BlockSpec(memory_space=pltpu.VMEM)
        dma = pltpu.SemaphoreType.DMA
        out_shape = (
            S((n_tok, d_model), BF16), S((n_tok, d_model), BF16), S((n_exp, d_model), F32),
            S((2, rows, f_loc), BF16), S((2, rows, f_loc), BF16),
            S((2, N_EP, block, d_model), BF16), S((2, N_EP, block, d_model), BF16),
        )
        scratch = [
            pltpu.VMEM((n_tok, d_model), BF16), pltpu.VMEM((n_tok, d_model), BF16),
            pltpu.VMEM(w_in.shape, BF16), pltpu.VMEM(w_out.shape, BF16),
            pltpu.VMEM((2 * rows, n_tok), BF16), pltpu.VMEM((n_exp, n_tok), F32),
            pltpu.VMEM((2, 2, N_EP, block, d_model), BF16), pltpu.VMEM((2, 2, N_EP, block, d_model), BF16),
            pltpu.VMEM((2, rows, f_loc), F32), pltpu.VMEM((2, rows, f_loc), BF16), pltpu.VMEM((2, rows, f_loc), BF16),
            pltpu.VMEM((4, 2, N_EP, block, half), F32), pltpu.VMEM((4, 2, block, half), F32),
            pltpu.VMEM((4, 2, block, half), F32), pltpu.VMEM((4, 2, 2, block, half), F32),
            pltpu.VMEM((4, block, d_model), BF16), pltpu.VMEM((4, N_EP, block, d_model), BF16),
            pltpu.VMEM((n_tok, d_model), BF16), pltpu.VMEM((n_tok, d_model), BF16),
            pltpu.VMEM((n_exp, d_model), F32), pltpu.VMEM((3, n_exp, d_model), F32), pltpu.VMEM((n_exp, d_model), F32),
            dma((6,)), dma((7,)), dma((2, 2, 3)), dma((2, 2, 3)), dma((4, 2, 3)), dma((4, 2, 3)),
            dma((4,)), dma((4, 3)), dma((4, 4)), dma((4, 2)), dma((3,)), dma((3,)),
        ]
        out, dx, dwg, h, da, xr, dyr = pl.pallas_call(
            functools.partial(moe_kernel, cap),
            out_shape=out_shape,
            in_specs=[vmem_spec, vmem_spec, any_spec, any_spec, any_spec, any_spec],
            out_specs=(any_spec,) * 7,
            scratch_shapes=scratch,
            compiler_params=pltpu.CompilerParams(collective_id=0, has_side_effects=True, vmem_limit_bytes=56 * 2**20),
        )(expert_ids.reshape(1, n_tok), w_router, tokens, grad_out, w_in, w_out)
        out, dx, dwi, dwo, dwg = pl.pallas_call(
            functools.partial(grads_kernel, cap),
            out_shape=(
                S((n_tok, d_model), BF16), S((n_tok, d_model), BF16),
                S((n_loc, d_model, f_loc), F32), S((n_loc, f_loc, d_model), F32), S((d_model, n_exp), F32),
            ),
            in_specs=[vmem_spec] * 7,
            out_specs=(vmem_spec, vmem_spec, any_spec, any_spec, vmem_spec),
            scratch_shapes=[pltpu.VMEM((8, d_model, f_loc), F32), dma((8,))],
            compiler_params=pltpu.CompilerParams(vmem_limit_bytes=56 * 2**20),
        )(h, da, xr, dyr, out, dx, dwg)
        return out, dx, dwi, dwo, dwg

    in_specs = (row_spec, row_spec, P(None, None), P("ep", None, "tp"), P("ep", "tp", None), P(("dp", "ep")))
    out_specs = (row_spec, row_spec, P(("dp", "ep"), None, "tp"), P(("dp", "ep"), "tp", None), P("dp", None))
    return jax.shard_map(local_block, mesh=mesh, in_specs=in_specs, out_specs=out_specs, check_vma=False)
```

```python
import functools

import jax
import jax.numpy as jnp
from jax import lax
from jax.experimental import pallas as pl
from jax.experimental.pallas import tpu as pltpu
from jax.sharding import PartitionSpec as P

MESH = pl.DeviceIdType.MESH
F32, BF16 = jnp.float32, jnp.bfloat16
GELU_C = 0.7978845608028654
GELU_K = 0.044715
N_EP, N_TP, N_PAIR, N_BACK = 4, 4, 2, 4


def dot(a, b, dims=((1,), (0,))):
    return lax.dot_general(a, b, (dims, ((), ())), preferred_element_type=F32)


def pair_masks(rows, block, cap):
    row = lax.broadcasted_iota(jnp.int32, (rows, 1), 0)
    first = lax.rem(row, block) < cap
    return jnp.where(first, 1.0, 0.0).astype(BF16), jnp.where(first, 0.0, 1.0).astype(BF16)


def moe_kernel(
    cap,
    ids_hbm, wg_hbm, x_hbm, gy_hbm, wi_hbm, wo_hbm,
    out_v, dx_v, dwg_v, dwi_v, dwo_v,
    ids_ref, wg_ref, x_v, gy_v, wi_v, wo_v,
    onehot_slots, router_v, send_v, recv_v, act_v, h_v, da_v,
    part_v, rs_in, red_v, slots_v,
    dwg_part, dwg_in,
    load_sem, sent_sem, disp_recv, rs_recv, hop_recv, ag_recv, wg_recv,
):
    block = 2 * cap
    rows = N_EP * block
    n_tok, d_model = x_v.shape
    n_exp = wg_ref.shape[0]
    half = d_model // 2
    z, j = lax.axis_index("tp"), lax.axis_index("ep")
    right, left = lax.rem(z + 1, N_TP), lax.rem(z + N_TP - 1, N_TP)
    ep_peer = [lax.rem(j + k, N_EP) for k in range(N_EP)]

    def remote(kind, src, dst, rsem, **dev):
        return pltpu.make_async_remote_copy(
            src_ref=src, dst_ref=dst, send_sem=sent_sem.at[kind], recv_sem=rsem, device_id=dev, device_id_type=MESH
        )

    def wait_bytes(ref, sem):
        pltpu.make_async_copy(ref, ref, sem).wait()

    load_x = pltpu.make_async_copy(x_hbm, x_v, load_sem.at[0])
    load_gy = pltpu.make_async_copy(gy_hbm, gy_v, load_sem.at[1])
    load_wi = [pltpu.make_async_copy(wi_hbm.at[pl.ds(2 * p, 2)], wi_v.at[pl.ds(2 * p, 2)], load_sem.at[2 + p]) for p in range(2)]
    load_wo = [pltpu.make_async_copy(wo_hbm.at[pl.ds(2 * p, 2)], wo_v.at[pl.ds(2 * p, 2)], load_sem.at[4 + p]) for p in range(2)]
    load_ids = pltpu.make_async_copy(ids_hbm, ids_ref, load_sem.at[6])
    load_wg = pltpu.make_async_copy(wg_hbm, wg_ref, load_sem.at[7])
    for load in (load_ids, load_x, load_wg, load_gy):
        load.start()

    barrier = pltpu.get_barrier_semaphore()
    for dev in [{"tp": right}, {"tp": left}] + [{"ep": ep_peer[k]} for k in range(1, N_EP)]:
        pl.semaphore_signal(barrier, inc=1, device_id=dev, device_id_type=MESH)

    for p in range(2):
        load_wi[p].start()
        load_wo[p].start()

    load_ids.wait()
    ids = ids_ref[...]
    chosen = ids == lax.broadcasted_iota(jnp.int32, (n_exp, n_tok), 0)
    onehot = jnp.where(chosen, 1.0, 0.0)
    before = lax.broadcasted_iota(jnp.int32, (n_tok, n_tok), 0) < lax.broadcasted_iota(jnp.int32, (n_tok, n_tok), 1)
    counts = dot(onehot.astype(BF16), jnp.where(before, 1.0, 0.0).astype(BF16))
    pos = jnp.sum(counts * onehot, axis=0, keepdims=True)
    base = ((ids >> 1) & 1) * rows + (ids >> 2) * block + (ids & 1) * cap
    slot = jnp.where(pos < cap, base.astype(F32) + pos, -1.0)
    slot_iota = lax.broadcasted_iota(jnp.int32, (2 * rows, n_tok), 0).astype(F32)
    onehot_slots[...] = jnp.where(slot_iota == slot, 1.0, 0.0).astype(BF16)

    def dispatch(t, tok_rows):
        packed = dot(onehot_slots[...], tok_rows).astype(BF16)
        send_v[t] = packed.reshape(2, N_EP, block, d_model)

    def disp_copy(t, p, k):
        return remote(
            0, send_v.at[t, p, ep_peer[k]], recv_v.at[t, p, j], disp_recv.at[t, p], ep=ep_peer[k]
        )

    def start_dispatch(t):
        for p in range(N_PAIR):
            for k in (2, 1, 3):
                disp_copy(t, p, k).start()
        for p in range(N_PAIR):
            recv_v[t, p, j] = send_v[t, p, j]

    def route_x():
        load_x.wait()
        dispatch(0, x_v[...])

    def route_dy():
        load_wg.wait()
        logits = dot(wg_ref[...], x_v[...], ((1,), (1,)))
        expd = jnp.exp(logits - jnp.max(logits, axis=0, keepdims=True))
        prob = expd / jnp.sum(expd, axis=0, keepdims=True)
        gate_row = jnp.sum(jnp.where(chosen, prob, 0.0), axis=0, keepdims=True)
        router_v[...] = prob * (onehot - gate_row)
        gate = jnp.transpose(jnp.broadcast_to(gate_row, (128, n_tok)))[:, :1]
        load_gy.wait()
        dispatch(1, (gate * gy_v[...].astype(F32)).astype(BF16))
        return gate

    def meet():
        pl.semaphore_wait(barrier, 5)

    def step(name, f, *a):
        with jax.named_scope(name + "".join(map(str, a))):
            return f(*a)

    step("route_x", route_x)
    step("meet", meet)
    start_dispatch(0)
    gate_v = step("route_dy", route_dy)
    start_dispatch(1)

    mask0, mask1 = pair_masks(rows, block, cap)

    def wait_rows(t, p):
        wait_bytes(recv_v.at[t, p, pl.ds(0, N_EP - 1)], disp_recv.at[t, p])
        return recv_v[t, p].reshape(rows, d_model)

    def pair_dot(lhs, w_ref, p, dims=((1,), (0,))):
        return dot(lhs * mask0, w_ref[2 * p], dims) + dot(lhs * mask1, w_ref[2 * p + 1], dims)

    place = [z, N_TP - 1 - z]
    ahead, behind = [right, left], [left, right]

    def rs_copy(i, h, q):
        return remote(1, part_v.at[i, h, q], rs_in.at[i, h, q], rs_recv.at[i, h, q], tp=ahead[h])

    def rs_start(i, part):
        part_v[i, 0] = part[:, :half].reshape(N_EP, block, half)
        part_v[i, 1] = part[:, half:].reshape(N_EP, block, half)
        for h in (0, 1):
            @pl.when(place[h] == 0)
            def _():
                for q in range(N_EP):
                    rs_copy(i, h, q).start()

    def rs_relay(at, i, q):
        for h in (0, 1):
            @pl.when(place[h] == at)
            def _():
                rs_copy(i, h, q).wait_recv()
                part_v[i, h, q] = part_v[i, h, q] + rs_in[i, h, q]
                rs_copy(i, h, q).start()

    def hop_copy(i, h, q):
        return remote(2, red_v.at[i, q], slots_v.at[i, h, j], hop_recv.at[i], ep=q)

    def rs_final(i, q):
        for h in (0, 1):
            @pl.when(place[h] == N_TP - 1)
            def _():
                rs_copy(i, h, q).wait_recv()
                red_v[i, q] = (part_v[i, h, q] + rs_in[i, h, q]).astype(BF16)

                @pl.when(j != q)
                def _():
                    hop_copy(i, h, q).start()

                @pl.when(j == q)
                def _():
                    slots_v[i, h, j] = red_v[i, q]

    def ag_copy(i, h, n):
        part = slots_v.at[i, h, pl.ds(n * (N_EP // N_BACK), N_EP // N_BACK)]
        return remote(3, part, part, ag_recv.at[i, h, n], tp=behind[h])

    def ag_root(i, q):
        for h in (0, 1):
            @pl.when((place[h] == N_TP - 1) & (j == q))
            def _():
                wait_bytes(slots_v.at[i, h, pl.ds(0, N_EP - 1)], hop_recv.at[i])
                for n in range(N_BACK):
                    ag_copy(i, h, n).start()

    def ag_forward(at, i, n):
        for h in (0, 1):
            @pl.when(place[h] == at)
            def _():
                ag_copy(i, h, n).wait_recv()
                ag_copy(i, h, n).start()

    def ag_last(i):
        for h in (0, 1):
            @pl.when(place[h] == 0)
            def _():
                for n in range(N_BACK):
                    ag_copy(i, h, n).wait_recv()

    def forward(p):
        load_wi[p].wait()
        xr = wait_rows(0, p)
        a = pair_dot(xr, wi_v, p)
        act_v[p] = a
        h = (0.5 * a * (1.0 + jnp.tanh(GELU_C * (a + GELU_K * a * a * a)))).astype(BF16)
        h_v[p] = h
        load_wo[p].wait()
        rs_start(p, pair_dot(h, wo_v, p))

    def backward_act(p):
        dyr = wait_rows(1, p)
        dh = pair_dot(dyr, wo_v, p, ((1,), (1,)))
        a = act_v[p]
        a2 = a * a
        th = jnp.tanh(GELU_C * (a + GELU_K * a2 * a))
        slope = 0.5 * (1.0 + th) + 0.5 * a * (1.0 - th * th) * (GELU_C * (1.0 + 3.0 * GELU_K * a2))
        da_v[p] = (dh * slope).astype(BF16)

    def backward_in(p):
        rs_start(2 + p, pair_dot(da_v[p], wi_v, p, ((1,), (1,))))

    def combine(t):
        halves = [
            jnp.concatenate([slots_v[2 * t + p, h].reshape(rows, half) for p in range(N_PAIR)], axis=0) for h in (0, 1)
        ]
        return dot(onehot_slots[...], jnp.concatenate(halves, axis=1), ((0,), (0,)))

    def weight_grad(n):
        e = n // 2
        p, mask = e // 2, (mask0, mask1)[e % 2]
        if n % 2 == 0:
            dwo_v[e] = dot(h_v[p] * mask, recv_v[1, p].reshape(rows, d_model), ((0,), (0,)))
        else:
            dwi_v[e] = dot(recv_v[0, p].reshape(rows, d_model) * mask, da_v[p], ((0,), (0,)))

    def first(k):
        step("relay1_", rs_relay, 1, k // 4, k % 4)

    def second(k):
        step("relay2_", rs_relay, 2, k // 4, k % 4)

    def last(k):
        step("final_", rs_final, k // 4, k % 4)

    step("forward", forward, 0)
    step("forward", forward, 1)
    first(0)
    step("bwd_act", backward_act, 0)
    first(1)
    step("bwd_in", backward_in, 0)
    first(2)
    second(0)
    step("bwd_act", backward_act, 1)
    first(3)
    second(1)
    step("bwd_in", backward_in, 1)

    def back(at, i, pieces=range(N_BACK)):
        for n in pieces:
            step(f"ag_fwd{at}_", ag_forward, at, i, n)

    for k in range(4, 16):
        first(k)
        second(k - 2)
        if 6 <= k < 14:
            step("weight_grad", weight_grad, k - 6)
    back(2, 0, [0, 1])
    second(14)
    back(2, 0, [2, 3])
    second(15)
    for k in range(16):
        last(k)
        if k >= 2:
            step("ag_root", ag_root, (k - 2) // 4, (k - 2) % 4)
    step("ag_root", ag_root, 3, 2)
    step("ag_root", ag_root, 3, 3)
    for n in range(N_BACK):
        back(2, 1, [n])
        back(1, 0, [n])
    for n in range(N_BACK):
        back(2, 2, [n])
        back(1, 1, [n])
    step("ag_last", ag_last, 0)
    step("ag_last", ag_last, 1)

    def wg_copy(k):
        return remote(4, dwg_part, dwg_in.at[k - 1], wg_recv, ep=ep_peer[k])

    def finish_y():
        y_tok = combine(0)
        out_v[...] = (gate_v * y_tok).astype(BF16)
        d_gate = jnp.sum(gy_v[...].astype(F32) * y_tok, axis=1, keepdims=True)
        d_gate_row = jnp.transpose(jnp.broadcast_to(d_gate, (n_tok, 128)))[:1]
        d_logits = d_gate_row * router_v[...]
        dwg_part[...] = dot(d_logits.astype(BF16), x_v[...])
        for k in range(1, N_EP):
            wg_copy(k).start()
        return dot(jnp.transpose(d_logits).astype(BF16), wg_ref[...])

    def finish_wg():
        wait_bytes(dwg_in, wg_recv)
        dwg_v[...] = (dwg_part[...] + dwg_in[1]) + (dwg_in[0] + dwg_in[2])

    def finish_s():
        dx_v[...] = (combine(1) + router_grad).astype(BF16)

    router_grad = step("finish_y", finish_y)
    for n in range(N_BACK):
        back(2, 3, [n])
        back(1, 2, [n])
    step("finish_wg", finish_wg)
    back(1, 3)
    step("ag_last", ag_last, 2)
    step("ag_last", ag_last, 3)
    step("finish_s", finish_s)

    def drain():
        wait_bytes(part_v.at[pl.ds(0, N_EP - 1), 0], sent_sem.at[0])
        wait_bytes(dwg_in, sent_sem.at[4])

        @pl.when((z == 0) | (z == N_TP - 1))
        def _():
            wait_bytes(part_v.at[:, 0], sent_sem.at[1])
            wait_bytes(red_v.at[:, pl.ds(0, N_EP - 1)], sent_sem.at[2])
            wait_bytes(slots_v.at[:, 0], sent_sem.at[3])

        @pl.when((z != 0) & (z != N_TP - 1))
        def _():
            wait_bytes(part_v, sent_sem.at[1])
            wait_bytes(slots_v, sent_sem.at[3])

    step("drain", drain)


def store_kernel(out_v, dx_v, dwg_v, dwi_v, dwo_v, out_hbm, dx_hbm, dwg_hbm, dwi_hbm, dwo_hbm, sem):
    pairs = [(dwi_v.at[e], dwi_hbm.at[e]) for e in range(4)] + [(dwo_v.at[e], dwo_hbm.at[e]) for e in range(4)]
    pairs += [(out_v, out_hbm), (dx_v, dx_hbm), (dwg_v, dwg_hbm)]
    copies = [pltpu.make_async_copy(src, dst, sem.at[n]) for n, (src, dst) in enumerate(pairs)]
    for cp in copies:
        cp.start()
    for cp in copies:
        cp.wait()


def solution(mesh):
    row_spec = P(("dp", "ep"), None)

    def local_block(tokens, grad_out, w_router, w_in, w_out, expert_ids):
        n_tok, d_model = tokens.shape
        n_exp = w_router.shape[1]
        n_loc, _, f_loc = w_in.shape
        cap = (6 * n_tok + 5 * n_exp - 1) // (5 * n_exp)
        block, rows, half = 2 * cap, 8 * cap, d_model // 2
        S = jax.ShapeDtypeStruct
        any_spec, vmem_spec = pl.BlockSpec(memory_space=pl.ANY), pl.BlockSpec(memory_space=pltpu.VMEM)
        dma = pltpu.SemaphoreType.DMA
        out_shape = (
            S((n_tok, d_model), BF16), S((n_tok, d_model), BF16), S((n_exp, d_model), F32),
            S((n_loc, d_model, f_loc), F32), S((n_loc, f_loc, d_model), F32),
        )
        held = tuple(pltpu.VMEM(s.shape, s.dtype) for s in out_shape)
        scratch = [
            pltpu.VMEM((1, n_tok), jnp.int32), pltpu.VMEM((n_exp, d_model), BF16),
            pltpu.VMEM((n_tok, d_model), BF16), pltpu.VMEM((n_tok, d_model), BF16),
            pltpu.VMEM(w_in.shape, BF16), pltpu.VMEM(w_out.shape, BF16),
            pltpu.VMEM((2 * rows, n_tok), BF16), pltpu.VMEM((n_exp, n_tok), F32),
            pltpu.VMEM((2, 2, N_EP, block, d_model), BF16), pltpu.VMEM((2, 2, N_EP, block, d_model), BF16),
            pltpu.VMEM((2, rows, f_loc), F32), pltpu.VMEM((2, rows, f_loc), BF16), pltpu.VMEM((2, rows, f_loc), BF16),
            pltpu.VMEM((4, 2, N_EP, block, half), F32), pltpu.VMEM((4, 2, N_EP, block, half), F32),
            pltpu.VMEM((4, N_EP, block, half), BF16), pltpu.VMEM((4, 2, N_EP, block, half), BF16),
            pltpu.VMEM((n_exp, d_model), F32), pltpu.VMEM((3, n_exp, d_model), F32),
            dma((8,)), dma((5,)), dma((2, 2)), dma((4, 2, N_EP)), dma((4,)), dma((4, 2, N_BACK)), dma,
        ]
        results = pl.pallas_call(
            functools.partial(moe_kernel, cap),
            out_shape=held,
            in_specs=[any_spec] * 6,
            out_specs=(vmem_spec,) * 5,
            scratch_shapes=scratch,
            compiler_params=pltpu.CompilerParams(collective_id=0, has_side_effects=True, vmem_limit_bytes=24 * 2**20),
        )(*[
            pltpu.with_memory_space_constraint(r, pltpu.HBM)
            for r in (expert_ids.reshape(1, n_tok), w_router.T, tokens, grad_out, w_in, w_out)
        ])
        out, dx, dwg, dwi, dwo = pl.pallas_call(
            store_kernel,
            out_shape=out_shape,
            in_specs=[any_spec] * 5,
            out_specs=(any_spec,) * 5,
            scratch_shapes=[dma((11,))],
            compiler_params=pltpu.CompilerParams(vmem_limit_bytes=2**20),
        )(*[pltpu.with_memory_space_constraint(r, pltpu.VMEM) for r in results])
        return out, dx, dwi, dwo, dwg.T

    in_specs = (row_spec, row_spec, P(None, None), P("ep", None, "tp"), P("ep", "tp", None), P(("dp", "ep")))
    out_specs = (row_spec, row_spec, P(("dp", "ep"), None, "tp"), P(("dp", "ep"), "tp", None), P("dp", None))
    return jax.shard_map(local_block, mesh=mesh, in_specs=in_specs, out_specs=out_specs, check_vma=False)
```

```python
import functools

import jax
import jax.numpy as jnp
from jax import lax
from jax.experimental import pallas as pl
from jax.experimental.pallas import tpu as pltpu
from jax.sharding import PartitionSpec as P

MESH = pl.DeviceIdType.MESH
F32, BF16 = jnp.float32, jnp.bfloat16
GELU_C = 0.7978845608028654
GELU_K = 0.044715
N_EP, N_TP, N_PAIR = 4, 4, 2


def dot(a, b, dims=((1,), (0,))):
    return lax.dot_general(a, b, (dims, ((), ())), preferred_element_type=F32)


def pair_masks(rows, block, cap):
    row = lax.broadcasted_iota(jnp.int32, (rows, 1), 0)
    first = lax.rem(row, block) < cap
    return jnp.where(first, 1.0, 0.0).astype(BF16), jnp.where(first, 0.0, 1.0).astype(BF16)


def moe_kernel(
    cap,
    ids_hbm, wg_hbm, x_hbm, gy_hbm, wi_hbm, wo_hbm,
    out_v, dx_v, dwg_v, dwi_v, dwo_v,
    ids_ref, wg_ref, x_v, gy_v, wi_v, wo_v,
    onehot_slots, router_v, send_v, recv_v, act_v, h_v, da_v,
    part_v, rs_in, red_v, slots_v,
    dwg_part, dwg_in,
    load_sem, sent_sem, disp_recv, rs_recv, hop_recv, turn_recv, back_recv, wg_recv,
):
    block = 2 * cap
    rows = N_EP * block
    n_tok, d_model = x_v.shape
    n_exp = wg_ref.shape[0]
    half = d_model // 2
    z, j = lax.axis_index("tp"), lax.axis_index("ep")
    right, left = lax.rem(z + 1, N_TP), lax.rem(z + N_TP - 1, N_TP)
    chip = j // 2
    near = j + 1 - 2 * lax.rem(j, 2)
    ep_peer = [near, lax.rem(j + 2, N_EP), lax.rem(near + 2, N_EP)]
    side = [2 * chip, 2 - 2 * chip]

    def remote(kind, src, dst, rsem, **dev):
        return pltpu.make_async_remote_copy(
            src_ref=src, dst_ref=dst, send_sem=sent_sem.at[kind], recv_sem=rsem, device_id=dev, device_id_type=MESH
        )

    def wait_bytes(ref, sem):
        pltpu.make_async_copy(ref, ref, sem).wait()

    load_x = pltpu.make_async_copy(x_hbm, x_v, load_sem.at[0])
    load_gy = pltpu.make_async_copy(gy_hbm, gy_v, load_sem.at[1])
    load_wi = [pltpu.make_async_copy(wi_hbm.at[pl.ds(2 * p, 2)], wi_v.at[pl.ds(2 * p, 2)], load_sem.at[2 + p]) for p in range(2)]
    load_wo = [pltpu.make_async_copy(wo_hbm.at[pl.ds(2 * p, 2)], wo_v.at[pl.ds(2 * p, 2)], load_sem.at[4 + p]) for p in range(2)]
    load_ids = pltpu.make_async_copy(ids_hbm, ids_ref, load_sem.at[6])
    load_wg = pltpu.make_async_copy(wg_hbm, wg_ref, load_sem.at[7])
    for load in (load_ids, load_x, load_wg, load_gy):
        load.start()

    barrier = pltpu.get_barrier_semaphore()
    pair_z = z + 1 - 2 * lax.rem(z, 2)
    at_end = (z == 0) | (z == N_TP - 1)

    def greet(**dev):
        pl.semaphore_signal(barrier, inc=1, device_id=dev, device_id_type=MESH)

    for peer in ep_peer:
        greet(ep=peer)
    for peer in [j] + ep_peer:
        greet(tp=pair_z, ep=peer)

    @pl.when(jnp.logical_not(at_end))
    def _():
        greet(tp=N_TP - 1 - z)

    for p in range(2):
        load_wi[p].start()
        load_wo[p].start()

    load_ids.wait()
    ids = ids_ref[...]
    chosen = ids == lax.broadcasted_iota(jnp.int32, (n_exp, n_tok), 0)
    onehot = jnp.where(chosen, 1.0, 0.0)
    before = lax.broadcasted_iota(jnp.int32, (n_tok, n_tok), 0) < lax.broadcasted_iota(jnp.int32, (n_tok, n_tok), 1)
    counts = dot(onehot.astype(BF16), jnp.where(before, 1.0, 0.0).astype(BF16))
    pos = jnp.sum(counts * onehot, axis=0, keepdims=True)
    base = ((ids >> 1) & 1) * rows + (ids >> 2) * block + (ids & 1) * cap
    slot = jnp.where(pos < cap, base.astype(F32) + pos, -1.0)
    slot_iota = lax.broadcasted_iota(jnp.int32, (2 * rows, n_tok), 0).astype(F32)
    onehot_slots[...] = jnp.where(slot_iota == slot, 1.0, 0.0).astype(BF16)

    def dispatch(t, tok_rows):
        packed = dot(onehot_slots[...], tok_rows).astype(BF16)
        send_v[t] = packed.reshape(2, N_EP, block, d_model)

    def disp_copy(t, p, k):
        peer = ep_peer[k]
        return remote(0, send_v.at[t, p, peer], recv_v.at[t, p, j], disp_recv.at[t, p, min(k, 1)], ep=peer)

    def start_dispatch(t):
        for p in range(N_PAIR):
            disp_copy(t, p, 0).start()
        for p in range(N_PAIR):
            for k in (1, 2):
                disp_copy(t, p, k).start()
        for p in range(N_PAIR):
            recv_v[t, p, j] = send_v[t, p, j]

    def route_x():
        load_x.wait()
        dispatch(0, x_v[...])

    def route_dy():
        load_wg.wait()
        logits = dot(wg_ref[...], x_v[...], ((1,), (1,)))
        expd = jnp.exp(logits - jnp.max(logits, axis=0, keepdims=True))
        prob = expd / jnp.sum(expd, axis=0, keepdims=True)
        gate_row = jnp.sum(jnp.where(chosen, prob, 0.0), axis=0, keepdims=True)
        router_v[...] = prob * (onehot - gate_row)
        gate = jnp.transpose(jnp.broadcast_to(gate_row, (128, n_tok)))[:, :1]
        load_gy.wait()
        dispatch(1, (gate * gy_v[...].astype(F32)).astype(BF16))
        return gate

    def meet():
        @pl.when(at_end)
        def _():
            pl.semaphore_wait(barrier, 7)

        @pl.when(jnp.logical_not(at_end))
        def _():
            pl.semaphore_wait(barrier, 8)

    def step(name, f, *a):
        with jax.named_scope(name + "".join(map(str, a))):
            return f(*a)

    step("route_x", route_x)
    step("meet", meet)
    start_dispatch(0)
    gate_v = step("route_dy", route_dy)
    start_dispatch(1)

    mask0, mask1 = pair_masks(rows, block, cap)
    part_rows = 2 * block

    def rows_from(t, p, far):
        return recv_v[t, p, pl.ds(side[far], 2)].reshape(part_rows, d_model)

    def wait_rows(t, p, far):
        wait_bytes(recv_v.at[t, p, pl.ds(0, 1 + far)], disp_recv.at[t, p, far])
        return rows_from(t, p, far)

    def all_rows(t, p):
        return jnp.concatenate([rows_from(t, p, far) for far in (0, 1)], axis=0)

    def pair_dot(lhs, w_ref, p, dims=((1,), (0,))):
        first, second = lhs * mask0[: lhs.shape[0]], lhs * mask1[: lhs.shape[0]]
        return dot(first, w_ref[2 * p], dims) + dot(second, w_ref[2 * p + 1], dims)

    place = [z, N_TP - 1 - z]
    ahead, behind = [right, left], [left, right]

    def rs_copy(i, h, q):
        return remote(1, part_v.at[i, h, q], rs_in.at[i, h, q], rs_recv.at[i, h, q], tp=ahead[h])

    def rs_start(i, far, part):
        where = pl.ds(side[far], 2)
        part_v[i, 0, where] = part[:, :half].reshape(2, block, half)
        part_v[i, 1, where] = part[:, half:].reshape(2, block, half)
        for h in (0, 1):
            @pl.when(place[h] == 0)
            def _():
                for b in range(2):
                    rs_copy(i, h, side[far] + b).start()

    def rs_relay(at, i, far, b):
        q = side[far] + b
        for h in (0, 1):
            @pl.when(place[h] == at)
            def _():
                rs_copy(i, h, q).wait_recv()
                part_v[i, h, q] = part_v[i, h, q] + rs_in[i, h, q]
                rs_copy(i, h, q).start()

    def hop_copy(i, h, q, far):
        return remote(2, red_v.at[i, q], slots_v.at[i, h, j], hop_recv.at[i, far], ep=q)

    def turn_copy(i, h, q, far):
        return remote(5, red_v.at[i, q], slots_v.at[i, h, j], turn_recv.at[i, far], tp=behind[h], ep=q)

    def rs_final(i, far, b):
        q = side[far] + b
        for h in (0, 1):
            @pl.when(place[h] == N_TP - 1)
            def _():
                rs_copy(i, h, q).wait_recv()
                red_v[i, q] = (part_v[i, h, q] + rs_in[i, h, q]).astype(BF16)
                turn_copy(i, h, q, far).start()
                if far:
                    hop_copy(i, h, q, far).start()
                else:
                    @pl.when(j != q)
                    def _():
                        hop_copy(i, h, q, far).start()

                    @pl.when(j == q)
                    def _():
                        slots_v[i, h, j] = red_v[i, q]

    def hop_wait(i):
        for h in (0, 1):
            @pl.when(place[h] == N_TP - 1)
            def _():
                for far in (0, 1):
                    wait_bytes(slots_v.at[i, h, pl.ds(0, 1 + far)], hop_recv.at[i, far])

    def back_copy(i, h, far):
        part = slots_v.at[i, h, pl.ds(side[far], 2)]
        return remote(3, part, part, back_recv.at[i, far], tp=behind[h])

    def back_first(i, far):
        for h in (0, 1):
            @pl.when(place[h] == 2)
            def _():
                wait_bytes(slots_v.at[i, h, pl.ds(0, 2)], turn_recv.at[i, far])
                back_copy(i, h, far).start()

    def back_second(i, far):
        for h in (0, 1):
            @pl.when(place[h] == 1)
            def _():
                back_copy(i, h, far).wait_recv()
                back_copy(i, h, far).start()

    def back_last(i, far):
        for h in (0, 1):
            @pl.when(place[h] == 0)
            def _():
                back_copy(i, h, far).wait_recv()

    def by_token(t):
        halves = [
            jnp.concatenate([slots_v[2 * t + p, h].reshape(rows, half) for p in range(N_PAIR)], axis=0) for h in (0, 1)
        ]
        return dot(onehot_slots[...], jnp.concatenate(halves, axis=1), ((0,), (0,)))

    def forward(p, far):
        if far == 0:
            load_wi[p].wait()
        a = pair_dot(wait_rows(0, p, far), wi_v, p)
        act_v[p, far] = a
        h = (0.5 * a * (1.0 + jnp.tanh(GELU_C * (a + GELU_K * a * a * a)))).astype(BF16)
        h_v[p, far] = h
        if far == 0:
            load_wo[p].wait()
        rs_start(p, far, pair_dot(h, wo_v, p))

    def backward_act(p):
        wait_rows(1, p, 0)
        wait_rows(1, p, 1)
        dh = pair_dot(all_rows(1, p), wo_v, p, ((1,), (1,)))
        a = act_v[p].reshape(rows, -1)
        a2 = a * a
        th = jnp.tanh(GELU_C * (a + GELU_K * a2 * a))
        slope = 0.5 * (1.0 + th) + 0.5 * a * (1.0 - th * th) * (GELU_C * (1.0 + 3.0 * GELU_K * a2))
        da_v[p] = (dh * slope).astype(BF16)

    def backward_in(p):
        part = pair_dot(da_v[p], wi_v, p, ((1,), (1,)))
        for far in (0, 1):
            rs_start(2 + p, far, part[far * part_rows : (far + 1) * part_rows])

    def weight_grad(n):
        e = n // 2
        p, mask = e // 2, (mask0, mask1)[e % 2]
        if n % 2 == 0:
            dwo_v[e] = dot(h_v[p].reshape(rows, -1) * mask, all_rows(1, p), ((0,), (0,)))
        else:
            dwi_v[e] = dot(all_rows(0, p) * mask, da_v[p], ((0,), (0,)))

    def first(k):
        step("relay1_", rs_relay, 1, *chunks[k])

    def second(k):
        step("relay2_", rs_relay, 2, *chunks[k])

    units = [(0, 0), (1, 0), (0, 1), (1, 1), (2, 0), (2, 1), (3, 0), (3, 1)]
    chunks = [(i, far, b) for i, far in units for b in range(2)]

    step("forward", forward, 0, 0)
    step("forward", forward, 1, 0)
    first(0)
    step("forward", forward, 0, 1)
    first(1)
    first(2)
    second(0)
    step("forward", forward, 1, 1)
    first(3)
    second(1)
    first(4)
    step("bwd_act", backward_act, 0)
    second(2)
    first(5)
    step("bwd_in", backward_in, 0)
    second(3)
    first(6)
    step("bwd_act", backward_act, 1)
    second(4)
    first(7)
    step("bwd_in", backward_in, 1)
    second(5)
    for k in range(8, 16):
        first(k)
        second(k - 2)
        step("weight_grad", weight_grad, k - 8)

    def turn(i, far):
        step("back1_", back_first, i, far)

    def back(i, far):
        step("back2_", back_second, i, far)

    second(14)
    turn(0, 0)
    second(15)
    for k in range(16):
        step("final_", rs_final, *chunks[k])
    for i, far in units[:4]:
        step("back3_", back_last, i, far)
    step("hop_", hop_wait, 0)
    step("hop_", hop_wait, 1)
    turn(1, 0)
    turn(0, 1)
    back(0, 0)
    turn(1, 1)
    back(1, 0)
    turn(2, 0)
    back(0, 1)
    turn(2, 1)
    back(1, 1)

    def wg_copy(k):
        return remote(4, dwg_part, dwg_in.at[k], wg_recv, ep=ep_peer[k])

    def finish_y():
        y_tok = by_token(0)
        out_v[...] = (gate_v * y_tok).astype(BF16)
        d_gate = jnp.sum(gy_v[...].astype(F32) * y_tok, axis=1, keepdims=True)
        d_gate_row = jnp.transpose(jnp.broadcast_to(d_gate, (n_tok, 128)))[:1]
        d_logits = d_gate_row * router_v[...]
        dwg_part[...] = dot(d_logits.astype(BF16), x_v[...])
        for k in range(3):
            wg_copy(k).start()
        return dot(jnp.transpose(d_logits).astype(BF16), wg_ref[...])

    def finish_wg():
        wait_bytes(dwg_in, wg_recv)
        dwg_v[...] = (dwg_part[...] + dwg_in[0]) + (dwg_in[1] + dwg_in[2])

    def finish_s():
        dx_v[...] = (by_token(1) + router_grad).astype(BF16)

    router_grad = step("finish_y", finish_y)
    turn(3, 0)
    back(2, 0)
    back(2, 1)
    turn(3, 1)
    back(3, 0)
    back(3, 1)
    for i, far in units[4:]:
        step("back3_", back_last, i, far)
    step("hop_", hop_wait, 2)
    step("hop_", hop_wait, 3)
    step("finish_s", finish_s)
    step("finish_wg", finish_wg)

    def drain():
        wait_bytes(part_v.at[pl.ds(0, N_EP - 1), 0], sent_sem.at[0])
        wait_bytes(dwg_in, sent_sem.at[4])

        @pl.when(at_end)
        def _():
            wait_bytes(part_v.at[:, 0], sent_sem.at[1])
            wait_bytes(red_v.at[:, pl.ds(0, N_EP - 1)], sent_sem.at[2])
            wait_bytes(red_v, sent_sem.at[5])

        @pl.when(jnp.logical_not(at_end))
        def _():
            wait_bytes(part_v, sent_sem.at[1])
            wait_bytes(slots_v, sent_sem.at[3])

    step("drain", drain)


def store_kernel(out_v, dx_v, dwg_v, dwi_v, dwo_v, out_hbm, dx_hbm, dwg_hbm, dwi_hbm, dwo_hbm, sem):
    pairs = [(dwi_v.at[e], dwi_hbm.at[e]) for e in range(4)] + [(dwo_v.at[e], dwo_hbm.at[e]) for e in range(4)]
    pairs += [(out_v, out_hbm), (dx_v, dx_hbm), (dwg_v, dwg_hbm)]
    copies = [pltpu.make_async_copy(src, dst, sem.at[n]) for n, (src, dst) in enumerate(pairs)]
    for cp in copies:
        cp.start()
    for cp in copies:
        cp.wait()


def solution(mesh):
    row_spec = P(("dp", "ep"), None)

    def local_block(tokens, grad_out, w_router, w_in, w_out, expert_ids):
        n_tok, d_model = tokens.shape
        n_exp = w_router.shape[1]
        n_loc, _, f_loc = w_in.shape
        cap = (6 * n_tok + 5 * n_exp - 1) // (5 * n_exp)
        block, rows, half = 2 * cap, 8 * cap, d_model // 2
        S = jax.ShapeDtypeStruct
        any_spec, vmem_spec = pl.BlockSpec(memory_space=pl.ANY), pl.BlockSpec(memory_space=pltpu.VMEM)
        dma = pltpu.SemaphoreType.DMA
        out_shape = (
            S((n_tok, d_model), BF16), S((n_tok, d_model), BF16), S((n_exp, d_model), F32),
            S((n_loc, d_model, f_loc), F32), S((n_loc, f_loc, d_model), F32),
        )
        held = tuple(pltpu.VMEM(s.shape, s.dtype) for s in out_shape)
        scratch = [
            pltpu.VMEM((1, n_tok), jnp.int32), pltpu.VMEM((n_exp, d_model), BF16),
            pltpu.VMEM((n_tok, d_model), BF16), pltpu.VMEM((n_tok, d_model), BF16),
            pltpu.VMEM(w_in.shape, BF16), pltpu.VMEM(w_out.shape, BF16),
            pltpu.VMEM((2 * rows, n_tok), BF16), pltpu.VMEM((n_exp, n_tok), F32),
            pltpu.VMEM((2, 2, N_EP, block, d_model), BF16), pltpu.VMEM((2, 2, N_EP, block, d_model), BF16),
            pltpu.VMEM((2, 2, rows // 2, f_loc), F32), pltpu.VMEM((2, 2, rows // 2, f_loc), BF16),
            pltpu.VMEM((2, rows, f_loc), BF16),
            pltpu.VMEM((4, 2, N_EP, block, half), F32), pltpu.VMEM((4, 2, N_EP, block, half), F32),
            pltpu.VMEM((4, N_EP, block, half), BF16), pltpu.VMEM((4, 2, N_EP, block, half), BF16),
            pltpu.VMEM((n_exp, d_model), F32), pltpu.VMEM((3, n_exp, d_model), F32),
            dma((8,)), dma((6,)), dma((2, 2, 2)), dma((4, 2, N_EP)), dma((4, 2)), dma((4, 2)), dma((4, 2)), dma,
        ]
        results = pl.pallas_call(
            functools.partial(moe_kernel, cap),
            out_shape=held,
            in_specs=[any_spec] * 6,
            out_specs=(vmem_spec,) * 5,
            scratch_shapes=scratch,
            compiler_params=pltpu.CompilerParams(collective_id=0, has_side_effects=True, vmem_limit_bytes=24 * 2**20),
        )(*[
            pltpu.with_memory_space_constraint(r, pltpu.HBM)
            for r in (expert_ids.reshape(1, n_tok), w_router.T, tokens, grad_out, w_in, w_out)
        ])
        out, dx, dwg, dwi, dwo = pl.pallas_call(
            store_kernel,
            out_shape=out_shape,
            in_specs=[any_spec] * 5,
            out_specs=(any_spec,) * 5,
            scratch_shapes=[dma((11,))],
            compiler_params=pltpu.CompilerParams(vmem_limit_bytes=2**20),
        )(*[pltpu.with_memory_space_constraint(r, pltpu.VMEM) for r in results])
        return out, dx, dwi, dwo, dwg.T

    in_specs = (row_spec, row_spec, P(None, None), P("ep", None, "tp"), P("ep", "tp", None), P(("dp", "ep")))
    out_specs = (row_spec, row_spec, P(("dp", "ep"), None, "tp"), P(("dp", "ep"), "tp", None), P("dp", None))
    return jax.shard_map(local_block, mesh=mesh, in_specs=in_specs, out_specs=out_specs, check_vma=False)
```

```python
import functools

import jax
import jax.numpy as jnp
from jax import lax
from jax.experimental import pallas as pl
from jax.experimental.pallas import tpu as pltpu
from jax.sharding import PartitionSpec as P

MESH = pl.DeviceIdType.MESH
F32, BF16 = jnp.float32, jnp.bfloat16
GELU_C = 0.7978845608028654
GELU_K = 0.044715
N_EP, N_TP, N_PAIR = 4, 4, 2


def dot(a, b, dims=((1,), (0,))):
    return lax.dot_general(a, b, (dims, ((), ())), preferred_element_type=F32)


def pair_masks(rows, block, cap):
    row = lax.broadcasted_iota(jnp.int32, (rows, 1), 0)
    first = lax.rem(row, block) < cap
    return jnp.where(first, 1.0, 0.0).astype(BF16), jnp.where(first, 0.0, 1.0).astype(BF16)


def half_by_token(onehot_slots, slots, first, h):
    n, width = onehot_slots.shape[0] // 2, slots.shape[-1]
    return dot(onehot_slots[...], jnp.concatenate([slots[first + p, h].reshape(n, width) for p in range(2)], axis=0), ((0,), (0,)))


def by_token(onehot_slots, slots, first):
    n, width = onehot_slots.shape[0] // 2, slots.shape[-1]
    halves = [jnp.concatenate([slots[first + p, h].reshape(n, width) for p in range(2)], axis=0) for h in (0, 1)]
    return dot(onehot_slots[...], jnp.concatenate(halves, axis=1), ((0,), (0,)))


def moe_kernel(
    cap,
    ids_hbm, wg_hbm, x_hbm, gy_hbm, wi_hbm, wo_hbm,
    gate_v, back_v, onehot_slots, rgrad_v, dwg_v, dwi_v, dwo_v,
    ids_ref, wg_ref, x_v, gy_v, wi_v, wo_v,
    router_v, send_v, recv_v, act_v, h_v, da_v, tmp_v,
    part_v, rs_in, red_v, slots_v,
    dwg_part, dwg_in, gate_rows,
    load_sem, sent_sem, disp_recv, rs_recv, hop_recv, turn_recv, back_recv, last_recv, wg_recv, gate_recv,
):
    block = 2 * cap
    rows = N_EP * block
    n_tok, d_model = x_v.shape
    n_exp = wg_ref.shape[0]
    half = d_model // 2
    z, j = lax.axis_index("tp"), lax.axis_index("ep")
    right, left = lax.rem(z + 1, N_TP), lax.rem(z + N_TP - 1, N_TP)
    chip = j // 2
    near = j + 1 - 2 * lax.rem(j, 2)
    ep_peer = [near, lax.rem(j + 2, N_EP), lax.rem(near + 2, N_EP)]
    side = [2 * chip, 2 - 2 * chip]

    def remote(kind, src, dst, rsem, **dev):
        return pltpu.make_async_remote_copy(
            src_ref=src, dst_ref=dst, send_sem=sent_sem.at[kind], recv_sem=rsem, device_id=dev, device_id_type=MESH
        )

    def wait_bytes(ref, sem):
        pltpu.make_async_copy(ref, ref, sem).wait()

    load_x = pltpu.make_async_copy(x_hbm, x_v, load_sem.at[0])
    load_gy = pltpu.make_async_copy(gy_hbm, gy_v, load_sem.at[1])
    load_wi = [pltpu.make_async_copy(wi_hbm.at[pl.ds(2 * p, 2)], wi_v.at[pl.ds(2 * p, 2)], load_sem.at[2 + p]) for p in range(2)]
    load_wo = [pltpu.make_async_copy(wo_hbm.at[pl.ds(2 * p, 2)], wo_v.at[pl.ds(2 * p, 2)], load_sem.at[4 + p]) for p in range(2)]
    load_ids = pltpu.make_async_copy(ids_hbm, ids_ref, load_sem.at[6])
    load_wg = pltpu.make_async_copy(wg_hbm, wg_ref, load_sem.at[7])
    for load in (load_ids, load_x, load_wg, load_gy):
        load.start()

    barrier = pltpu.get_barrier_semaphore()
    pair_z = z + 1 - 2 * lax.rem(z, 2)
    at_end = (z == 0) | (z == N_TP - 1)

    def greet(**dev):
        pl.semaphore_signal(barrier, inc=1, device_id=dev, device_id_type=MESH)

    for peer in ep_peer:
        greet(ep=peer)
    for peer in [j] + ep_peer:
        greet(tp=pair_z, ep=peer)

    @pl.when(jnp.logical_not(at_end))
    def _():
        greet(tp=N_TP - 1 - z)

    for p in range(2):
        load_wi[p].start()
        load_wo[p].start()

    load_ids.wait()
    ids = ids_ref[...]
    chosen = ids == lax.broadcasted_iota(jnp.int32, (n_exp, n_tok), 0)
    onehot = jnp.where(chosen, 1.0, 0.0)
    before = lax.broadcasted_iota(jnp.int32, (n_tok, n_tok), 0) < lax.broadcasted_iota(jnp.int32, (n_tok, n_tok), 1)
    counts = dot(onehot.astype(BF16), jnp.where(before, 1.0, 0.0).astype(BF16))
    pos = jnp.sum(counts * onehot, axis=0, keepdims=True)
    base = ((ids >> 1) & 1) * rows + (ids >> 2) * block + (ids & 1) * cap
    slot = jnp.where(pos < cap, base.astype(F32) + pos, -1.0)
    slot_iota = lax.broadcasted_iota(jnp.int32, (2 * rows, n_tok), 0).astype(F32)
    onehot_slots[...] = jnp.where(slot_iota == slot, 1.0, 0.0).astype(BF16)

    def dispatch(t, tok_rows):
        packed = dot(onehot_slots[...], tok_rows).astype(BF16)
        send_v[t] = packed.reshape(2, N_EP, block, d_model)

    def disp_copy(t, p, k):
        peer = ep_peer[k]
        return remote(0, send_v.at[t, p, peer], recv_v.at[t, p, j], disp_recv.at[t, p, min(k, 1)], ep=peer)

    def start_dispatch(t):
        for p in range(N_PAIR):
            disp_copy(t, p, 0).start()
        for p in range(N_PAIR):
            for k in (1, 2):
                disp_copy(t, p, k).start()

    def keep_own(t):
        for p in range(N_PAIR):
            recv_v[t, p, j] = send_v[t, p, j]

    def route_x():
        load_x.wait()
        dispatch(0, x_v[...])
        keep_own(0)

    def route_dy():
        load_wg.wait()
        logits = dot(wg_ref[...], x_v[...], ((1,), (1,)))
        expd = jnp.exp(logits - jnp.max(logits, axis=0, keepdims=True))
        prob = expd / jnp.sum(expd, axis=0, keepdims=True)
        gate_row = jnp.sum(jnp.where(chosen, prob, 0.0), axis=0, keepdims=True)
        router_v[...] = prob * (onehot - gate_row)
        gate_all = jnp.transpose(jnp.broadcast_to(gate_row, (128, n_tok)))
        gate_v[...] = gate_all
        gate = gate_all[:, :1]
        load_gy.wait()
        dispatch(1, (gate * gy_v[...].astype(F32)).astype(BF16))

    def meet():
        @pl.when(at_end)
        def _():
            pl.semaphore_wait(barrier, 7)

        @pl.when(jnp.logical_not(at_end))
        def _():
            pl.semaphore_wait(barrier, 8)

    def step(name, f, *a):
        with jax.named_scope(name + "".join(str(v) for v in a if isinstance(v, int))):
            return f(*a)

    mask0, mask1 = pair_masks(rows, block, cap)

    OWN, MATE, NEAR, FAR, ALL = (j, 1), (near, 1), (side[0], 2), (side[1], 2), (0, N_EP)

    def group(ref, p, g):
        return ref[p, pl.ds(*g)].reshape(g[1] * block, ref.shape[-1])

    def put(ref, p, g, value):
        ref[p, pl.ds(*g)] = value.reshape(g[1], block, value.shape[-1])

    def wait_rows(t, p, far):
        wait_bytes(recv_v.at[t, p, pl.ds(0, 1 + far)], disp_recv.at[t, p, far])

    def one_dot(lhs, w_ref, p, which, dims=((1,), (0,))):
        mask = (mask0, mask1)[which]
        return dot(lhs * mask[: lhs.shape[0]], w_ref[2 * p + which], dims)

    def pair_dot(lhs, w_ref, p):
        return one_dot(lhs, w_ref, p, 0) + one_dot(lhs, w_ref, p, 1)

    place = [z, N_TP - 1 - z]
    ahead, behind = [right, left], [left, right]

    def rs_copy(i, h, q):
        return remote(1, part_v.at[i, h, q], rs_in.at[i, h, q], rs_recv.at[i, h, q], tp=ahead[h])

    def rs_start(i, g, part):
        for h in (0, 1):
            part_v[i, h, pl.ds(*g)] = part[:, h * half : (h + 1) * half].reshape(g[1], block, half)
        for h in (0, 1):
            @pl.when(place[h] == 0)
            def _():
                for first, count in (NEAR, FAR) if g is ALL else (g,):
                    for b in range(count):
                        rs_copy(i, h, first + b).start()

    def rs_relay(at, i, q):
        for h in (0, 1):
            @pl.when(place[h] == at)
            def _():
                rs_copy(i, h, q).wait_recv()
                part_v[i, h, q] = part_v[i, h, q] + rs_in[i, h, q]
                rs_copy(i, h, q).start()

    def hop_copy(i, h, q, far):
        return remote(2, red_v.at[i, q], slots_v.at[i, h, j], hop_recv.at[i, far], ep=q)

    def turn_copy(i, h, q, far):
        return remote(5 if i < 3 else 7, red_v.at[i, q], slots_v.at[i, h, j], turn_recv.at[i, far], tp=behind[h], ep=q)

    def last_turn(h, q):
        return remote(7, red_v.at[3, q], slots_v.at[3, h, j], last_recv.at[0, lax.rem(j, 2)], tp=behind[h], ep=q)

    def last_back(h, b):
        part = slots_v.at[3, h, side[1] + b]
        return remote(8, part, part, last_recv.at[1, b], tp=behind[h])

    def last_first(b):
        for h in (0, 1):
            @pl.when(place[h] == 2)
            def _():
                wait_bytes(slots_v.at[3, h, 0], last_recv.at[0, b])
                last_back(h, b).start()

    def last_second(b):
        for h in (0, 1):
            @pl.when(place[h] == 1)
            def _():
                last_back(h, b).wait_recv()
                last_back(h, b).start()

    def last_last(b):
        for h in (0, 1):
            @pl.when(place[h] == 0)
            def _():
                last_back(h, b).wait_recv()

    def turn_start(i, far, q):
        for h in (0, 1):
            @pl.when(place[h] == N_TP - 1)
            def _():
                turn_copy(i, h, q, far).start()

    def sums_sent():
        @pl.when(at_end)
        def _():
            wait_bytes(part_v.at[:, 0], sent_sem.at[1])

    def rs_final(i, far, q, turn=True):
        for h in (0, 1):
            @pl.when(place[h] == N_TP - 1)
            def _():
                rs_copy(i, h, q).wait_recv()
                red_v[i, q] = (part_v[i, h, q] + rs_in[i, h, q]).astype(BF16)
                if (i, far) == (3, 1):
                    last_turn(h, q).start()
                elif turn:
                    turn_copy(i, h, q, far).start()
                if far:
                    hop_copy(i, h, q, far).start()
                else:
                    @pl.when(j != q)
                    def _():
                        hop_copy(i, h, q, far).start()

                    @pl.when(j == q)
                    def _():
                        slots_v[i, h, j] = red_v[i, q]

    def hop_wait(i):
        for far in (0, 1):
            wait_bytes(slots_v.at[i, 0, pl.ds(0, 1 + far)], hop_recv.at[i, far])

    def hop_wait_end(i):
        @pl.when(at_end)
        def _():
            hop_wait(i)

    def back_copy(i, h, far):
        part = slots_v.at[i, h, pl.ds(side[far], 2)]
        return remote(3 if i < 3 else 8, part, part, back_recv.at[i, far], tp=behind[h])

    def back_first(i, far):
        for h in (0, 1):
            @pl.when(place[h] == 2)
            def _():
                wait_bytes(slots_v.at[i, h, pl.ds(0, 2)], turn_recv.at[i, far])
                back_copy(i, h, far).start()

    def back_second(i, far):
        for h in (0, 1):
            @pl.when(place[h] == 1)
            def _():
                back_copy(i, h, far).wait_recv()
                back_copy(i, h, far).start()

    def back_last(i, far):
        for h in (0, 1):
            @pl.when(place[h] == 0)
            def _():
                back_copy(i, h, far).wait_recv()

    def gate_copy(h, at):
        tp = at if h == 0 else N_TP - 1 - at
        return remote(10, gate_rows.at[h], gate_rows.at[h], gate_recv.at[h], tp=tp)

    def gate_root():
        for h in (0, 1):
            @pl.when(place[h] == N_TP - 1)
            def _():
                hop_wait(0)
                hop_wait(1)
                y_tok = half_by_token(onehot_slots, slots_v, 0, h)
                part = jnp.sum(gy_v[:, h * half : (h + 1) * half].astype(F32) * y_tok, axis=1, keepdims=True)
                gate_rows[h] = jnp.transpose(jnp.broadcast_to(part, (n_tok, 128)))[:8]
                for at in range(N_TP - 1):
                    gate_copy(h, at).start()

    def wg_copy(k):
        return remote(4, dwg_part, dwg_in.at[k], wg_recv, ep=ep_peer[k])

    def router_back():
        for h in (0, 1):
            @pl.when(place[h] != N_TP - 1)
            def _():
                gate_copy(h, 0).wait_recv()
        d_logits = (gate_rows[0, :1] + gate_rows[1, :1]) * router_v[...]
        dwg_part[...] = dot(d_logits.astype(BF16), x_v[...])
        for k in range(3):
            wg_copy(k).start()
        rgrad_v[...] = dot(jnp.transpose(d_logits).astype(BF16), wg_ref[...])

    def forward_act(p, g):
        a = pair_dot(group(recv_v.at[0], p, g), wi_v, p)
        put(act_v, p, g, a)
        put(h_v, p, g, (0.5 * a * (1.0 + jnp.tanh(GELU_C * (a + GELU_K * a * a * a)))).astype(BF16))

    def forward_out(p, g):
        rs_start(p, g, pair_dot(group(h_v, p, g), wo_v, p))

    NT = ((1,), (1,))

    def backward_act0(p, g):
        put(tmp_v, 0, g, one_dot(group(recv_v.at[1], p, g), wo_v, p, 0, NT))

    def backward_act1(p, g):
        dh = group(tmp_v, 0, g) + one_dot(group(recv_v.at[1], p, g), wo_v, p, 1, NT)
        a = group(act_v, p, g)
        a2 = a * a
        th = jnp.tanh(GELU_C * (a + GELU_K * a2 * a))
        slope = 0.5 * (1.0 + th) + 0.5 * a * (1.0 - th * th) * (GELU_C * (1.0 + 3.0 * GELU_K * a2))
        put(da_v, p, g, (dh * slope).astype(BF16))

    def backward_in0(p, g):
        put(tmp_v, 1, g, one_dot(group(da_v, p, g), wi_v, p, 0, NT))

    def backward_in1(p, g):
        rs_start(2 + p, g, group(tmp_v, 1, g) + one_dot(group(da_v, p, g), wi_v, p, 1, NT))

    def weight_grad(n):
        e = n // 2
        p, mask = e // 2, (mask0, mask1)[e % 2]
        if n % 2 == 0:
            dwo_v[e] = dot(group(h_v, p, ALL) * mask, group(recv_v.at[1], p, ALL), ((0,), (0,)))
        else:
            dwi_v[e] = dot(group(recv_v.at[0], p, ALL) * mask, group(da_v, p, ALL), ((0,), (0,)))

    order = [(0, 0, OWN), (0, 0, MATE), (1, 0, NEAR), (2, 0, NEAR), (0, 1, FAR), (1, 1, FAR), (2, 1, FAR), (3, 0, NEAR), (3, 1, FAR)]
    chunks = [(i, far, g[0] + b) for i, far, g in order for b in range(g[1])]

    def relay(at, k):
        with jax.named_scope(f"relay{at}_{k}"):
            rs_relay(at, chunks[k][0], chunks[k][2])

    def wait_both(t, p):
        wait_rows(t, p, 0)
        wait_rows(t, p, 1)

    def own_act():
        load_wi[0].wait()
        forward_act(0, OWN)

    def own_out():
        load_wo[0].wait()
        forward_out(0, OWN)

    def start_mate():
        wait_rows(0, 0, 0)
        forward_act(0, MATE)
        forward_out(0, MATE)

    def near_next():
        load_wi[1].wait()
        wait_rows(0, 1, 0)
        forward_act(1, NEAR)

    def near_next_out():
        load_wo[1].wait()
        forward_out(1, NEAR)

    def back_units(p, g, wait):
        def head():
            wait()
            backward_act0(p, g)

        return [head] + [functools.partial(f, p, g) for f in (backward_act1, backward_in0, backward_in1)]

    def far_units(p):
        def head():
            wait_rows(0, p, 1)
            forward_act(p, FAR)

        return [head, functools.partial(forward_out, p, FAR)]

    step("route_x", route_x)
    step("meet", meet)
    start_dispatch(0)
    step("own_act", own_act)
    step("own_out", own_out)
    step("mate", start_mate)
    step("route_dy", route_dy)
    keep_own(1)
    start_dispatch(1)
    step("near1", near_next)
    step("near1_out", near_next_out)

    def timed(ready, lengths, units):
        return [(ready, length, f) for length, f in zip(lengths, units)]

    work = timed(7.0, (0.42, 0.62, 0.42, 0.62), back_units(0, NEAR, lambda: wait_rows(1, 0, 0)))
    work += timed(7.9, (0.62, 0.62), far_units(0)) + timed(11.0, (0.62, 0.62), far_units(1))
    work += timed(13.5, (0.42, 0.6, 0.42, 0.6), back_units(0, FAR, lambda: wait_rows(1, 0, 1)))
    work += timed(16.5, (0.47, 0.65, 0.47, 0.65), back_units(1, ALL, lambda: wait_both(1, 1)))
    work += timed(16.5, (0.61,) * 8, [functools.partial(weight_grad, n) for n in range(8)])
    relays = [(7.0 + 1.31 * k, 1, k) for k in range(16)] + [(10.4 + 1.31 * k, 2, k) for k in range(16)]
    relays = sorted(relays)[:-2]
    now, n_work = 7.2, 0
    while relays or work:
        due = relays[0][0] if relays else 1e9
        ready = work[0][0] if work else 1e9
        if work and ready <= now and (now + work[0][1] <= due + 0.15):
            step(f"work{n_work}", work[0][2])
            now += work.pop(0)[1]
            n_work += 1
        elif relays and due <= max(now, ready):
            relay(*relays.pop(0)[1:])
            now = max(now, due) + 0.1
        else:
            now = min(due, max(now, ready)) if ready > now else due

    def turn(i, far):
        step("back1_", back_first, i, far)

    def back(i, far):
        step("back2_", back_second, i, far)

    pieces = [(0, 0), (1, 0), (2, 0), (0, 1), (1, 1), (2, 1), (3, 0)]
    turn(*pieces[0])
    relay(2, 14)
    turn(*pieces[1])
    relay(2, 15)
    for k in range(16):
        step(f"final{k}_", rs_final, *chunks[k], k >= 6)
        if k == 5:
            step("sums_sent", sums_sent)
            for n in range(6):
                turn_start(*chunks[n])
        if k == 12:
            step("gate_root", gate_root)
    def finish_wg():
        wait_bytes(dwg_in, wg_recv)
        dwg_v[...] = (dwg_part[...] + dwg_in[0]) + (dwg_in[1] + dwg_in[2])

    def hand_over():
        back_v[...] = slots_v[...]

    for n in range(2, 7):
        turn(*pieces[n])
        back(*pieces[n - 2])
        if n == 5:
            step("router_back", router_back)
    back(*pieces[5])
    step("last_first", last_first, 0)
    step("last_first", last_first, 1)
    back(*pieces[6])
    step("last_second", last_second, 0)
    step("last_second", last_second, 1)
    for n in range(7):
        step("back3_", back_last, *pieces[n])
    step("last_last", last_last, 0)
    step("last_last", last_last, 1)
    step("hop_", hop_wait_end, 2)
    step("hop_", hop_wait_end, 3)
    step("hand_over", hand_over)
    step("finish_wg", finish_wg)

    def drain():
        wait_bytes(part_v.at[pl.ds(0, N_EP - 1), 0], sent_sem.at[0])
        wait_bytes(dwg_in, sent_sem.at[4])

        @pl.when(at_end)
        def _():
            wait_bytes(red_v.at[:, pl.ds(0, N_EP - 1)], sent_sem.at[2])
            wait_bytes(red_v.at[pl.ds(0, 3)], sent_sem.at[5])
            wait_bytes(red_v.at[0], sent_sem.at[7])
            wait_bytes(gate_rows.at[pl.ds(0, 3)], sent_sem.at[10])

        @pl.when(jnp.logical_not(at_end))
        def _():
            wait_bytes(part_v, sent_sem.at[1])
            wait_bytes(slots_v.at[pl.ds(0, 3)], sent_sem.at[3])
            wait_bytes(slots_v.at[0], sent_sem.at[8])

    step("drain", drain)


def store_kernel(
    gate_v, back_v, onehot_slots, rgrad_v, dwg_v, dwi_v, dwo_v, out_hbm, dx_hbm, dwg_hbm, dwi_hbm, dwo_hbm, out_v, dx_v, sem
):
    pairs = [(dwi_v.at[e], dwi_hbm.at[e]) for e in range(4)] + [(dwo_v.at[e], dwo_hbm.at[e]) for e in range(4)]
    pairs += [(dwg_v, dwg_hbm), (out_v, out_hbm), (dx_v, dx_hbm)]
    copies = [pltpu.make_async_copy(src, dst, sem.at[n]) for n, (src, dst) in enumerate(pairs)]
    for cp in copies[:-2]:
        cp.start()
    out_v[...] = (gate_v[:, :1] * by_token(onehot_slots, back_v, 0)).astype(BF16)
    copies[-2].start()
    dx_v[...] = (by_token(onehot_slots, back_v, 2) + rgrad_v[...]).astype(BF16)
    copies[-1].start()
    for cp in copies:
        cp.wait()


def solution(mesh):
    row_spec = P(("dp", "ep"), None)

    def local_block(tokens, grad_out, w_router, w_in, w_out, expert_ids):
        n_tok, d_model = tokens.shape
        n_exp = w_router.shape[1]
        n_loc, _, f_loc = w_in.shape
        cap = (6 * n_tok + 5 * n_exp - 1) // (5 * n_exp)
        block, rows, half = 2 * cap, 8 * cap, d_model // 2
        S = jax.ShapeDtypeStruct
        any_spec, vmem_spec = pl.BlockSpec(memory_space=pl.ANY), pl.BlockSpec(memory_space=pltpu.VMEM)
        dma = pltpu.SemaphoreType.DMA
        out_shape = (
            S((n_tok, d_model), BF16), S((n_tok, d_model), BF16), S((n_exp, d_model), F32),
            S((n_loc, d_model, f_loc), F32), S((n_loc, f_loc, d_model), F32),
        )
        handed = (
            S((n_tok, 128), F32), S((4, 2, N_EP, block, half), BF16), S((2 * rows, n_tok), BF16), S((n_tok, d_model), F32),
        ) + out_shape[2:]
        held = tuple(pltpu.VMEM(s.shape, s.dtype) for s in handed)
        scratch = [
            pltpu.VMEM((1, n_tok), jnp.int32), pltpu.VMEM((n_exp, d_model), BF16),
            pltpu.VMEM((n_tok, d_model), BF16), pltpu.VMEM((n_tok, d_model), BF16),
            pltpu.VMEM(w_in.shape, BF16), pltpu.VMEM(w_out.shape, BF16),
            pltpu.VMEM((n_exp, n_tok), F32),
            pltpu.VMEM((2, 2, N_EP, block, d_model), BF16), pltpu.VMEM((2, 2, N_EP, block, d_model), BF16),
            pltpu.VMEM((2, N_EP, block, f_loc), F32), pltpu.VMEM((2, N_EP, block, f_loc), BF16),
            pltpu.VMEM((2, N_EP, block, f_loc), BF16), pltpu.VMEM((2, N_EP, block, d_model), F32),
            pltpu.VMEM((4, 2, N_EP, block, half), F32), pltpu.VMEM((4, 2, N_EP, block, half), F32),
            pltpu.VMEM((4, N_EP, block, half), BF16), pltpu.VMEM((4, 2, N_EP, block, half), BF16),
            pltpu.VMEM((n_exp, d_model), F32), pltpu.VMEM((3, n_exp, d_model), F32), pltpu.VMEM((4, 8, n_tok), F32),
            dma((8,)), dma((11,)), dma((2, 2, 2)), dma((4, 2, N_EP)), dma((4, 2)), dma((4, 2)), dma((4, 2)), dma((2, 2)), dma, dma((2,)),
        ]
        results = pl.pallas_call(
            functools.partial(moe_kernel, cap),
            out_shape=held,
            in_specs=[any_spec] * 6,
            out_specs=(vmem_spec,) * 7,
            scratch_shapes=scratch,
            compiler_params=pltpu.CompilerParams(collective_id=0, has_side_effects=True, vmem_limit_bytes=24 * 2**20),
        )(*[
            pltpu.with_memory_space_constraint(r, pltpu.HBM)
            for r in (expert_ids.reshape(1, n_tok), w_router.T, tokens, grad_out, w_in, w_out)
        ])
        out, dx, dwg, dwi, dwo = pl.pallas_call(
            store_kernel,
            out_shape=out_shape,
            in_specs=[vmem_spec] * 7,
            out_specs=(any_spec,) * 5,
            scratch_shapes=[pltpu.VMEM((n_tok, d_model), BF16), pltpu.VMEM((n_tok, d_model), BF16), dma((11,))],
            compiler_params=pltpu.CompilerParams(vmem_limit_bytes=8 * 2**20),
        )(*[pltpu.with_memory_space_constraint(r, pltpu.VMEM) for r in results])
        return out, dx, dwi, dwo, dwg.T

    in_specs = (row_spec, row_spec, P(None, None), P("ep", None, "tp"), P("ep", "tp", None), P(("dp", "ep")))
    out_specs = (row_spec, row_spec, P(("dp", "ep"), None, "tp"), P(("dp", "ep"), "tp", None), P("dp", None))
    return jax.shard_map(local_block, mesh=mesh, in_specs=in_specs, out_specs=out_specs, check_vma=False)
```

```python
import functools

import jax
import jax.numpy as jnp
from jax import lax
from jax.experimental import pallas as pl
from jax.experimental.pallas import tpu as pltpu
from jax.sharding import PartitionSpec as P

MESH = pl.DeviceIdType.MESH
F32, BF16 = jnp.float32, jnp.bfloat16
GELU_C = 0.7978845608028654
GELU_K = 0.044715
N_EP, N_TP, N_PAIR = 4, 4, 2
HALVES = range(2)


def dot(a, b, dims=((1,), (0,))):
    return lax.dot_general(a, b, (dims, ((), ())), preferred_element_type=F32)


def pair_masks(rows, block, cap):
    row = lax.broadcasted_iota(jnp.int32, (rows, 1), 0)
    first = lax.rem(row, block) < cap
    return jnp.where(first, 1.0, 0.0).astype(BF16), jnp.where(first, 0.0, 1.0).astype(BF16)


def half_by_token(onehot_slots, slots, first, h):
    n, width = onehot_slots.shape[0] // 2, slots.shape[-1]
    return dot(onehot_slots[...], jnp.concatenate([slots[first + p, h].reshape(n, width) for p in range(2)], axis=0), ((0,), (0,)))


def by_token(onehot_slots, slots, first):
    n, width = onehot_slots.shape[0] // 2, slots.shape[-1]
    halves = [jnp.concatenate([slots[first + p, h].reshape(n, width) for p in range(2)], axis=0) for h in HALVES]
    return dot(onehot_slots[...], jnp.concatenate(halves, axis=1), ((0,), (0,)))


def moe_kernel(
    cap,
    ids_hbm, wg_hbm, x_hbm, gy_hbm, wi_hbm, wo_hbm,
    gate_v, back_v, onehot_slots, rgrad_v, dwg_v, dwi_v, dwo_v,
    ids_ref, wg_ref, x_v, gy_v, wi_v, wo_v,
    router_v, send_v, recv_v, act_v, h_v, da_v, tmp_v,
    part_v, rs_in, red_v, slots_v,
    dwg_part, dwg_in, gate_rows,
    load_sem, sent_sem, disp_recv, rs_recv, hop_recv, turn_recv, back_recv, last_recv, wg_recv, gate_recv,
):
    block = 2 * cap
    rows = N_EP * block
    n_tok, d_model = x_v.shape
    n_exp = wg_ref.shape[0]
    half = d_model // 2
    z, j = lax.axis_index("tp"), lax.axis_index("ep")
    right, left = lax.rem(z + 1, N_TP), lax.rem(z + N_TP - 1, N_TP)
    chip = j // 2
    near = j + 1 - 2 * lax.rem(j, 2)
    ep_peer = [near, lax.rem(j + 2, N_EP), lax.rem(near + 2, N_EP)]
    side = [2 * chip, 2 - 2 * chip]

    def remote(kind, src, dst, rsem, **dev):
        return pltpu.make_async_remote_copy(
            src_ref=src, dst_ref=dst, send_sem=sent_sem.at[kind], recv_sem=rsem, device_id=dev, device_id_type=MESH
        )

    def wait_bytes(ref, sem):
        pltpu.make_async_copy(ref, ref, sem).wait()

    load_x = pltpu.make_async_copy(x_hbm, x_v, load_sem.at[0])
    load_gy = pltpu.make_async_copy(gy_hbm, gy_v, load_sem.at[1])
    load_wi = [pltpu.make_async_copy(wi_hbm.at[pl.ds(2 * p, 2)], wi_v.at[pl.ds(2 * p, 2)], load_sem.at[2 + p]) for p in range(2)]
    load_wo = [pltpu.make_async_copy(wo_hbm.at[pl.ds(2 * p, 2)], wo_v.at[pl.ds(2 * p, 2)], load_sem.at[4 + p]) for p in range(2)]
    load_ids = pltpu.make_async_copy(ids_hbm, ids_ref, load_sem.at[6])
    load_wg = pltpu.make_async_copy(wg_hbm, wg_ref, load_sem.at[7])
    for load in (load_ids, load_x, load_wi[0], load_wo[0], load_wg, load_gy, load_wi[1], load_wo[1]):
        load.start()

    barrier = pltpu.get_barrier_semaphore()
    pair_z = z + 1 - 2 * lax.rem(z, 2)
    at_end = (z == 0) | (z == N_TP - 1)

    def greet(**dev):
        pl.semaphore_signal(barrier, inc=1, device_id=dev, device_id_type=MESH)

    for peer in ep_peer:
        greet(ep=peer)
    for peer in [j] + ep_peer:
        greet(tp=pair_z, ep=peer)

    @pl.when(jnp.logical_not(at_end))
    def _():
        greet(tp=N_TP - 1 - z)

    load_ids.wait()
    ids = ids_ref[...]
    chosen = ids == lax.broadcasted_iota(jnp.int32, (n_exp, n_tok), 0)
    onehot = jnp.where(chosen, 1.0, 0.0)
    before = lax.broadcasted_iota(jnp.int32, (n_tok, n_tok), 0) < lax.broadcasted_iota(jnp.int32, (n_tok, n_tok), 1)
    counts = dot(onehot.astype(BF16), jnp.where(before, 1.0, 0.0).astype(BF16))
    pos = jnp.sum(counts * onehot, axis=0, keepdims=True)
    base = ((ids >> 1) & 1) * rows + (ids >> 2) * block + (ids & 1) * cap
    slot = jnp.where(pos < cap, base.astype(F32) + pos, -1.0)
    slot_iota = lax.broadcasted_iota(jnp.int32, (2 * rows, n_tok), 0).astype(F32)
    onehot_slots[...] = jnp.where(slot_iota == slot, 1.0, 0.0).astype(BF16)

    def dispatch(t, tok_rows):
        packed = dot(onehot_slots[...], tok_rows).astype(BF16)
        send_v[t] = packed.reshape(2, N_EP, block, d_model)

    def disp_copy(t, p, k):
        peer = ep_peer[k]
        return remote(0, send_v.at[t, p, peer], recv_v.at[t, p, j], disp_recv.at[t, p, min(k, 1)], ep=peer)

    def start_dispatch(t):
        for p in range(N_PAIR):
            disp_copy(t, p, 0).start()
        for p in range(N_PAIR):
            for k in (1, 2):
                disp_copy(t, p, k).start()

    def keep_own(t):
        for p in range(N_PAIR):
            recv_v[t, p, j] = send_v[t, p, j]

    def route_x():
        load_x.wait()
        dispatch(0, x_v[...])
        keep_own(0)

    def route_dy():
        load_wg.wait()
        logits = dot(wg_ref[...], x_v[...], ((1,), (1,)))
        expd = jnp.exp(logits - jnp.max(logits, axis=0, keepdims=True))
        prob = expd / jnp.sum(expd, axis=0, keepdims=True)
        gate_row = jnp.sum(jnp.where(chosen, prob, 0.0), axis=0, keepdims=True)
        router_v[...] = prob * (onehot - gate_row)
        gate_all = jnp.transpose(jnp.broadcast_to(gate_row, (128, n_tok)))
        gate_v[...] = gate_all
        gate = gate_all[:, :1]
        load_gy.wait()
        dispatch(1, (gate * gy_v[...].astype(F32)).astype(BF16))

    def meet():
        @pl.when(at_end)
        def _():
            pl.semaphore_wait(barrier, 7)

        @pl.when(jnp.logical_not(at_end))
        def _():
            pl.semaphore_wait(barrier, 8)

    def step(name, f, *a):
        with jax.named_scope(name + "".join(str(v) for v in a if isinstance(v, int))):
            return f(*a)

    mask0, mask1 = pair_masks(rows, block, cap)

    OWN, MATE, NEAR, FAR, ALL = (j, 1), (near, 1), (side[0], 2), (side[1], 2), (0, N_EP)

    def group(ref, p, g):
        return ref[p, pl.ds(*g)].reshape(g[1] * block, ref.shape[-1])

    def put(ref, p, g, value):
        ref[p, pl.ds(*g)] = value.reshape(g[1], block, value.shape[-1])

    def wait_rows(t, p, far):
        wait_bytes(recv_v.at[t, p, pl.ds(0, 1 + far)], disp_recv.at[t, p, far])

    def one_dot(lhs, w_ref, p, which, dims=((1,), (0,))):
        mask = (mask0, mask1)[which]
        return dot(lhs * mask[: lhs.shape[0]], w_ref[2 * p + which], dims)

    def pair_dot(lhs, w_ref, p):
        return one_dot(lhs, w_ref, p, 0) + one_dot(lhs, w_ref, p, 1)

    place = [z, N_TP - 1 - z]
    ahead, behind = [right, left], [left, right]

    def rs_copy(i, h, q):
        return remote(1, part_v.at[i, h, q], rs_in.at[i, h, q], rs_recv.at[i, h, q], tp=ahead[h])

    def rs_start(i, g, part):
        for h in HALVES:
            part_v[i, h, pl.ds(*g)] = part[:, h * half : (h + 1) * half].reshape(g[1], block, half)
        for h in HALVES:
            @pl.when(place[h] == 0)
            def _():
                for first, count in (NEAR, FAR) if g is ALL else (g,):
                    for b in range(count):
                        rs_copy(i, h, first + b).start()

    def rs_relay(at, i, q):
        for h in HALVES:
            @pl.when(place[h] == at)
            def _():
                rs_copy(i, h, q).wait_recv()
                part_v[i, h, q] = part_v[i, h, q] + rs_in[i, h, q]
                rs_copy(i, h, q).start()

    def hop_copy(i, h, q, far):
        return remote(2, red_v.at[i, q], slots_v.at[i, h, j], hop_recv.at[i, far], ep=q)

    def turn_copy(i, h, q, far):
        return remote(5 if i < 3 else 7, red_v.at[i, q], slots_v.at[i, h, j], turn_recv.at[i, far], tp=behind[h], ep=q)

    def last_turn(h, q):
        return remote(7, red_v.at[3, q], slots_v.at[3, h, j], last_recv.at[0, lax.rem(j, 2)], tp=behind[h], ep=q)

    def last_back(h, b):
        part = slots_v.at[3, h, side[1] + b]
        return remote(8, part, part, last_recv.at[1, b], tp=behind[h])

    def last_first(b):
        for h in HALVES:
            @pl.when(place[h] == 2)
            def _():
                wait_bytes(slots_v.at[3, h, 0], last_recv.at[0, b])
                last_back(h, b).start()

    def last_second(b):
        for h in HALVES:
            @pl.when(place[h] == 1)
            def _():
                last_back(h, b).wait_recv()
                last_back(h, b).start()

    def last_last(b):
        for h in HALVES:
            @pl.when(place[h] == 0)
            def _():
                last_back(h, b).wait_recv()

    def rs_final(i, far, q):
        for h in HALVES:
            @pl.when(place[h] == N_TP - 1)
            def _():
                rs_copy(i, h, q).wait_recv()
                red_v[i, q] = (part_v[i, h, q] + rs_in[i, h, q]).astype(BF16)
                if (i, far) == (3, 1):
                    last_turn(h, q).start()
                else:
                    turn_copy(i, h, q, far).start()
                if far:
                    hop_copy(i, h, q, far).start()
                else:
                    @pl.when(j != q)
                    def _():
                        hop_copy(i, h, q, far).start()

                    @pl.when(j == q)
                    def _():
                        slots_v[i, h, j] = red_v[i, q]

    def hop_wait(i):
        for far in HALVES:
            wait_bytes(slots_v.at[i, 0, pl.ds(0, 1 + far)], hop_recv.at[i, far])

    def hop_wait_end(i):
        @pl.when(at_end)
        def _():
            hop_wait(i)

    def back_copy(i, h, far):
        part = slots_v.at[i, h, pl.ds(side[far], 2)]
        return remote(3 if i < 3 else 8, part, part, back_recv.at[i, far], tp=behind[h])

    def back_first(i, far):
        for h in HALVES:
            @pl.when(place[h] == 2)
            def _():
                wait_bytes(slots_v.at[i, h, pl.ds(0, 2)], turn_recv.at[i, far])
                back_copy(i, h, far).start()

    def back_second(i, far):
        for h in HALVES:
            @pl.when(place[h] == 1)
            def _():
                back_copy(i, h, far).wait_recv()
                back_copy(i, h, far).start()

    def back_last(i, far):
        for h in HALVES:
            @pl.when(place[h] == 0)
            def _():
                back_copy(i, h, far).wait_recv()

    def gate_copy(h, at):
        tp = at if h == 0 else N_TP - 1 - at
        return remote(10, gate_rows.at[h], gate_rows.at[h], gate_recv.at[h], tp=tp)

    def gate_root():
        for h in HALVES:
            @pl.when(place[h] == N_TP - 1)
            def _():
                hop_wait(0)
                hop_wait(1)
                y_tok = half_by_token(onehot_slots, slots_v, 0, h)
                part = jnp.sum(gy_v[:, h * half : (h + 1) * half].astype(F32) * y_tok, axis=1, keepdims=True)
                gate_rows[h] = jnp.transpose(jnp.broadcast_to(part, (n_tok, 128)))[:8]
                for at in range(N_TP - 1):
                    gate_copy(h, at).start()

    def wg_copy(k):
        return remote(4, dwg_part, dwg_in.at[k], wg_recv, ep=ep_peer[k])

    def router_back():
        for h in HALVES:
            @pl.when(place[h] != N_TP - 1)
            def _():
                gate_copy(h, 0).wait_recv()
        d_logits = (gate_rows[0, :1] + gate_rows[1, :1]) * router_v[...]
        dwg_part[...] = dot(d_logits.astype(BF16), x_v[...])
        for k in range(3):
            wg_copy(k).start()
        rgrad_v[...] = dot(jnp.transpose(d_logits).astype(BF16), wg_ref[...])

    def forward_act(p, g):
        a = pair_dot(group(recv_v.at[0], p, g), wi_v, p)
        put(act_v, p, g, a)
        put(h_v, p, g, (0.5 * a * (1.0 + jnp.tanh(GELU_C * (a + GELU_K * a * a * a)))).astype(BF16))

    def forward_out(p, g):
        rs_start(p, g, pair_dot(group(h_v, p, g), wo_v, p))

    NT = ((1,), (1,))

    def backward_act0(p, g):
        put(tmp_v, 0, g, one_dot(group(recv_v.at[1], p, g), wo_v, p, 0, NT))

    def backward_act1(p, g):
        dh = group(tmp_v, 0, g) + one_dot(group(recv_v.at[1], p, g), wo_v, p, 1, NT)
        a = group(act_v, p, g)
        a2 = a * a
        th = jnp.tanh(GELU_C * (a + GELU_K * a2 * a))
        slope = 0.5 * (1.0 + th) + 0.5 * a * (1.0 - th * th) * (GELU_C * (1.0 + 3.0 * GELU_K * a2))
        put(da_v, p, g, (dh * slope).astype(BF16))

    def backward_in0(p, g):
        put(tmp_v, 1, g, one_dot(group(da_v, p, g), wi_v, p, 0, NT))

    def backward_in1(p, g):
        rs_start(2 + p, g, group(tmp_v, 1, g) + one_dot(group(da_v, p, g), wi_v, p, 1, NT))

    def weight_grad(n):
        e = n // 2
        p, mask = e // 2, (mask0, mask1)[e % 2]
        if n % 2 == 0:
            dwo_v[e] = dot(group(h_v, p, ALL) * mask, group(recv_v.at[1], p, ALL), ((0,), (0,)))
        else:
            dwi_v[e] = dot(group(recv_v.at[0], p, ALL) * mask, group(da_v, p, ALL), ((0,), (0,)))

    order = [(0, 0, OWN), (0, 0, MATE), (1, 0, NEAR), (2, 0, NEAR), (0, 1, FAR), (1, 1, FAR), (2, 1, FAR), (3, 0, NEAR), (3, 1, FAR)]
    chunks = [(i, far, g[0] + b) for i, far, g in order for b in range(g[1])]

    pieces = [(0, 0), (1, 0), (2, 0), (0, 1), (1, 1), (2, 1), (3, 0)]

    def relay(at, k):
        with jax.named_scope(f"relay{at}_{k}"):
            if at == 3:
                back_first(*pieces[k])
            else:
                rs_relay(at, chunks[k][0], chunks[k][2])

    def wait_both(t, p):
        wait_rows(t, p, 0)
        wait_rows(t, p, 1)

    def own_act():
        load_wi[0].wait()
        forward_act(0, OWN)

    def own_out():
        load_wo[0].wait()
        forward_out(0, OWN)

    def start_mate():
        wait_rows(0, 0, 0)
        forward_act(0, MATE)
        forward_out(0, MATE)

    def near_next():
        load_wi[1].wait()
        wait_rows(0, 1, 0)
        forward_act(1, NEAR)

    def near_next_out():
        load_wo[1].wait()
        forward_out(1, NEAR)

    def back_units(p, g, wait):
        def head():
            wait()
            backward_act0(p, g)

        return [head] + [functools.partial(f, p, g) for f in (backward_act1, backward_in0, backward_in1)]

    def far_units(p):
        def head():
            wait_rows(0, p, 1)
            forward_act(p, FAR)

        return [head, functools.partial(forward_out, p, FAR)]

    step("route_x", route_x)
    step("meet", meet)
    start_dispatch(0)
    step("own_act", own_act)
    step("own_out", own_out)
    step("mate", start_mate)
    step("route_dy", route_dy)
    keep_own(1)
    start_dispatch(1)
    step("near1", near_next)
    step("near1_out", near_next_out)

    def timed(ready, lengths, units):
        return [(ready, length, f) for length, f in zip(lengths, units)]

    work = timed(7.0, (0.42, 0.62, 0.42, 0.62), back_units(0, NEAR, lambda: wait_rows(1, 0, 0)))
    work += timed(7.9, (0.62, 0.62), far_units(0)) + timed(11.0, (0.62, 0.62), far_units(1))
    work += timed(13.5, (0.42, 0.6, 0.42, 0.6), back_units(0, FAR, lambda: wait_rows(1, 0, 1)))
    work += timed(16.5, (0.47, 0.65, 0.47, 0.65), back_units(1, ALL, lambda: wait_both(1, 1)))
    work += timed(16.5, (0.61,) * 8, [functools.partial(weight_grad, n) for n in range(8)])
    relays = [(7.0 + 1.33 * k, 1, k) for k in range(16)] + [(11.4 + 1.33 * k, 2, k) for k in range(16)]
    relays = sorted(relays + [(28.4 + 1.31 * k, 3, k) for k in range(3)])
    now, n_work = 7.2, 0
    while relays or work:
        due = relays[0][0] if relays else 1e9
        ready = work[0][0] if work else 1e9
        if work and ready <= now and (now + work[0][1] <= due + 0.15):
            step(f"work{n_work}", work[0][2])
            now += work.pop(0)[1]
            n_work += 1
        elif relays and due <= max(now, ready):
            relay(*relays.pop(0)[1:])
            now = max(now, due) + 0.1
        else:
            now = min(due, max(now, ready)) if ready > now else due

    def turn(i, far):
        step("back1_", back_first, i, far)

    def back(i, far):
        step("back2_", back_second, i, far)

    for k in range(16):
        step(f"final{k}_", rs_final, *chunks[k])
        if k == 12:
            step("gate_root", gate_root)
    def finish_wg():
        wait_bytes(dwg_in, wg_recv)
        dwg_v[...] = (dwg_part[...] + dwg_in[0]) + (dwg_in[1] + dwg_in[2])

    def hand_over():
        back_v[...] = slots_v[...]

    for n in range(2, 7):
        if n > 2:
            turn(*pieces[n])
        back(*pieces[n - 2])
        if n == 5:
            step("router_back", router_back)
    back(*pieces[5])
    step("last_first", last_first, 0)
    step("last_first", last_first, 1)
    back(*pieces[6])
    step("last_second", last_second, 0)
    step("last_second", last_second, 1)
    for n in range(7):
        step("back3_", back_last, *pieces[n])
    step("last_last", last_last, 0)
    step("last_last", last_last, 1)
    step("hop_", hop_wait_end, 2)
    step("hop_", hop_wait_end, 3)
    step("hand_over", hand_over)
    step("finish_wg", finish_wg)

    def drain():
        wait_bytes(part_v.at[pl.ds(0, N_EP - 1), 0], sent_sem.at[0])
        wait_bytes(dwg_in, sent_sem.at[4])

        @pl.when(at_end)
        def _():
            wait_bytes(part_v.at[:, 0], sent_sem.at[1])
            wait_bytes(red_v.at[:, pl.ds(0, N_EP - 1)], sent_sem.at[2])
            wait_bytes(red_v.at[pl.ds(0, 3)], sent_sem.at[5])
            wait_bytes(red_v.at[0], sent_sem.at[7])
            wait_bytes(gate_rows.at[pl.ds(0, 3)], sent_sem.at[10])

        @pl.when(jnp.logical_not(at_end))
        def _():
            wait_bytes(part_v, sent_sem.at[1])
            wait_bytes(slots_v.at[pl.ds(0, 3)], sent_sem.at[3])
            wait_bytes(slots_v.at[0], sent_sem.at[8])

    step("drain", drain)


def store_kernel(
    gate_v, back_v, onehot_slots, rgrad_v, dwg_v, dwi_v, dwo_v, out_hbm, dx_hbm, dwg_hbm, dwi_hbm, dwo_hbm, out_v, dx_v, sem
):
    pairs = [(dwi_v.at[e], dwi_hbm.at[e]) for e in range(4)] + [(dwo_v.at[e], dwo_hbm.at[e]) for e in range(4)]
    pairs += [(dwg_v, dwg_hbm), (out_v, out_hbm), (dx_v, dx_hbm)]
    copies = [pltpu.make_async_copy(src, dst, sem.at[n]) for n, (src, dst) in enumerate(pairs)]
    for cp in copies[:-2]:
        cp.start()
    out_v[...] = (gate_v[:, :1] * by_token(onehot_slots, back_v, 0)).astype(BF16)
    copies[-2].start()
    dx_v[...] = (by_token(onehot_slots, back_v, 2) + rgrad_v[...]).astype(BF16)
    copies[-1].start()
    for cp in copies:
        cp.wait()


def solution(mesh):
    row_spec = P(("dp", "ep"), None)

    def local_block(tokens, grad_out, w_router, w_in, w_out, expert_ids):
        n_tok, d_model = tokens.shape
        n_exp = w_router.shape[1]
        n_loc, _, f_loc = w_in.shape
        cap = (6 * n_tok + 5 * n_exp - 1) // (5 * n_exp)
        block, rows, half = 2 * cap, 8 * cap, d_model // 2
        S = jax.ShapeDtypeStruct
        any_spec, vmem_spec = pl.BlockSpec(memory_space=pl.ANY), pl.BlockSpec(memory_space=pltpu.VMEM)
        dma = pltpu.SemaphoreType.DMA
        out_shape = (
            S((n_tok, d_model), BF16), S((n_tok, d_model), BF16), S((n_exp, d_model), F32),
            S((n_loc, d_model, f_loc), F32), S((n_loc, f_loc, d_model), F32),
        )
        handed = (
            S((n_tok, 128), F32), S((4, 2, N_EP, block, half), BF16), S((2 * rows, n_tok), BF16), S((n_tok, d_model), F32),
        ) + out_shape[2:]
        held = tuple(pltpu.VMEM(s.shape, s.dtype) for s in handed)
        scratch = [
            pltpu.VMEM((1, n_tok), jnp.int32), pltpu.VMEM((n_exp, d_model), BF16),
            pltpu.VMEM((n_tok, d_model), BF16), pltpu.VMEM((n_tok, d_model), BF16),
            pltpu.VMEM(w_in.shape, BF16), pltpu.VMEM(w_out.shape, BF16),
            pltpu.VMEM((n_exp, n_tok), F32),
            pltpu.VMEM((2, 2, N_EP, block, d_model), BF16), pltpu.VMEM((2, 2, N_EP, block, d_model), BF16),
            pltpu.VMEM((2, N_EP, block, f_loc), F32), pltpu.VMEM((2, N_EP, block, f_loc), BF16),
            pltpu.VMEM((2, N_EP, block, f_loc), BF16), pltpu.VMEM((2, N_EP, block, d_model), F32),
            pltpu.VMEM((4, 2, N_EP, block, half), F32), pltpu.VMEM((4, 2, N_EP, block, half), F32),
            pltpu.VMEM((4, N_EP, block, half), BF16), pltpu.VMEM((4, 2, N_EP, block, half), BF16),
            pltpu.VMEM((n_exp, d_model), F32), pltpu.VMEM((3, n_exp, d_model), F32), pltpu.VMEM((4, 8, n_tok), F32),
            dma((8,)), dma((11,)), dma((2, 2, 2)), dma((4, 2, N_EP)), dma((4, 2)), dma((4, 2)), dma((4, 2)), dma((2, 2)), dma, dma((2,)),
        ]
        results = pl.pallas_call(
            functools.partial(moe_kernel, cap),
            out_shape=held,
            in_specs=[any_spec] * 6,
            out_specs=(vmem_spec,) * 7,
            scratch_shapes=scratch,
            compiler_params=pltpu.CompilerParams(collective_id=0, has_side_effects=True, vmem_limit_bytes=24 * 2**20),
        )(*[
            pltpu.with_memory_space_constraint(r, pltpu.HBM)
            for r in (expert_ids.reshape(1, n_tok), w_router.T, tokens, grad_out, w_in, w_out)
        ])
        out, dx, dwg, dwi, dwo = pl.pallas_call(
            store_kernel,
            out_shape=out_shape,
            in_specs=[vmem_spec] * 7,
            out_specs=(any_spec,) * 5,
            scratch_shapes=[pltpu.VMEM((n_tok, d_model), BF16), pltpu.VMEM((n_tok, d_model), BF16), dma((11,))],
            compiler_params=pltpu.CompilerParams(vmem_limit_bytes=8 * 2**20),
        )(*[pltpu.with_memory_space_constraint(r, pltpu.VMEM) for r in results])
        return out, dx, dwi, dwo, dwg.T

    in_specs = (row_spec, row_spec, P(None, None), P("ep", None, "tp"), P("ep", "tp", None), P(("dp", "ep")))
    out_specs = (row_spec, row_spec, P(("dp", "ep"), None, "tp"), P(("dp", "ep"), "tp", None), P("dp", None))
    return jax.shard_map(local_block, mesh=mesh, in_specs=in_specs, out_specs=out_specs, check_vma=False)
```

```python
import functools

import jax
import jax.numpy as jnp
from jax import lax
from jax.experimental import pallas as pl
from jax.experimental.pallas import tpu as pltpu
from jax.sharding import PartitionSpec as P

MESH = pl.DeviceIdType.MESH
F32, BF16 = jnp.float32, jnp.bfloat16
GELU_C = 0.7978845608028654
GELU_K = 0.044715
N_EP, N_TP, N_PAIR = 4, 4, 2
HALVES = range(2)
LAST = 3


def dot(a, b, dims=((1,), (0,))):
    return lax.dot_general(a, b, (dims, ((), ())), preferred_element_type=F32)


def pair_masks(rows, block, cap):
    row = lax.broadcasted_iota(jnp.int32, (rows, 1), 0)
    first = lax.rem(row, block) < cap
    return jnp.where(first, 1.0, 0.0).astype(BF16), jnp.where(first, 0.0, 1.0).astype(BF16)


def half_by_token(onehot_slots, slots, first, h):
    n, width = onehot_slots.shape[0] // 2, slots.shape[-1]
    return dot(onehot_slots[...], jnp.concatenate([slots[first + p, h].reshape(n, width) for p in range(2)], axis=0), ((0,), (0,)))


def by_token(onehot_slots, slots, first):
    n, width = onehot_slots.shape[0] // 2, slots.shape[-1]
    halves = [jnp.concatenate([slots[first + p, h].reshape(n, width) for p in range(2)], axis=0) for h in HALVES]
    return dot(onehot_slots[...], jnp.concatenate(halves, axis=1), ((0,), (0,)))


def moe_kernel(
    cap,
    ids_hbm, wg_hbm, x_hbm, gy_hbm, wi_hbm, wo_hbm,
    gate_v, back_v, onehot_slots, rgrad_v, dwg_v, dwi_v, dwo_v,
    ids_ref, wg_ref, x_v, gy_v, wi_v, wo_v,
    router_v, send_v, recv_v, act_v, h_v, da_v, tmp_v,
    part_v, rs_in, red_v, slots_v,
    dwg_part, dwg_in, gate_rows,
    load_sem, sent_sem, disp_recv, rs_recv, hop_recv, turn_recv, back_recv, last_recv, wg_recv, gate_recv,
):
    block = 2 * cap
    rows = N_EP * block
    n_tok, d_model = x_v.shape
    n_exp = wg_ref.shape[0]
    half = d_model // 2
    z, j = lax.axis_index("tp"), lax.axis_index("ep")
    right, left = lax.rem(z + 1, N_TP), lax.rem(z + N_TP - 1, N_TP)
    chip = j // 2
    near = j + 1 - 2 * lax.rem(j, 2)
    ep_peer = [near, lax.rem(j + 2, N_EP), lax.rem(near + 2, N_EP)]
    side = [2 * chip, 2 - 2 * chip]

    def remote(kind, src, dst, rsem, **dev):
        return pltpu.make_async_remote_copy(
            src_ref=src, dst_ref=dst, send_sem=sent_sem.at[kind], recv_sem=rsem, device_id=dev, device_id_type=MESH
        )

    def wait_bytes(ref, sem):
        pltpu.make_async_copy(ref, ref, sem).wait()

    load_x = pltpu.make_async_copy(x_hbm, x_v, load_sem.at[0])
    load_gy = pltpu.make_async_copy(gy_hbm, gy_v, load_sem.at[1])
    def load_weights(src, dst, first, count, n):
        return pltpu.make_async_copy(src.at[pl.ds(first, count)], dst.at[pl.ds(first, count)], load_sem.at[n])

    load_wi = [load_weights(wi_hbm, wi_v, *a) for a in ((0, 1, 2), (1, 1, 3), (2, 2, 4))]
    load_wo = [load_weights(wo_hbm, wo_v, *a) for a in ((0, 1, 8), (1, 1, 9), (2, 2, 5))]
    load_ids = pltpu.make_async_copy(ids_hbm, ids_ref, load_sem.at[6])
    load_wg = pltpu.make_async_copy(wg_hbm, wg_ref, load_sem.at[7])
    for load in (load_ids, load_x, *load_wi[:2], *load_wo[:2], load_wg, load_gy, load_wi[2], load_wo[2]):
        load.start()

    barrier = pltpu.get_barrier_semaphore()
    pair_z = z + 1 - 2 * lax.rem(z, 2)
    at_end = (z == 0) | (z == N_TP - 1)

    def greet(**dev):
        pl.semaphore_signal(barrier, inc=1, device_id=dev, device_id_type=MESH)

    for peer in ep_peer:
        greet(ep=peer)
    for peer in [j] + ep_peer:
        greet(tp=pair_z, ep=peer)

    @pl.when(jnp.logical_not(at_end))
    def _():
        greet(tp=N_TP - 1 - z)

    load_ids.wait()
    ids = ids_ref[...]
    chosen = ids == lax.broadcasted_iota(jnp.int32, (n_exp, n_tok), 0)
    onehot = jnp.where(chosen, 1.0, 0.0)
    before = lax.broadcasted_iota(jnp.int32, (n_tok, n_tok), 0) < lax.broadcasted_iota(jnp.int32, (n_tok, n_tok), 1)
    counts = dot(onehot.astype(BF16), jnp.where(before, 1.0, 0.0).astype(BF16))
    pos = jnp.sum(counts * onehot, axis=0, keepdims=True)
    base = ((ids >> 1) & 1) * rows + (ids >> 2) * block + (ids & 1) * cap
    slot = jnp.where(pos < cap, base.astype(F32) + pos, -1.0)
    slot_iota = lax.broadcasted_iota(jnp.int32, (2 * rows, n_tok), 0).astype(F32)
    onehot_slots[...] = jnp.where(slot_iota == slot, 1.0, 0.0).astype(BF16)

    def dispatch(t, tok_rows):
        packed = dot(onehot_slots[...], tok_rows).astype(BF16)
        send_v[t] = packed.reshape(2, N_EP, block, d_model)

    def disp_copy(t, p, k):
        peer = ep_peer[k]
        return remote(0, send_v.at[t, p, peer], recv_v.at[t, p, j], disp_recv.at[t, p, min(k, 1)], ep=peer)

    def start_dispatch(t):
        for p in range(N_PAIR):
            disp_copy(t, p, 0).start()
        for p in range(N_PAIR):
            for k in (1, 2):
                disp_copy(t, p, k).start()

    def keep_own(t):
        for p in range(N_PAIR):
            recv_v[t, p, j] = send_v[t, p, j]

    def route_x():
        load_x.wait()
        dispatch(0, x_v[...])
        keep_own(0)

    def route_dy():
        load_wg.wait()
        logits = dot(wg_ref[...], x_v[...], ((1,), (1,)))
        expd = jnp.exp(logits - jnp.max(logits, axis=0, keepdims=True))
        prob = expd / jnp.sum(expd, axis=0, keepdims=True)
        gate_row = jnp.sum(jnp.where(chosen, prob, 0.0), axis=0, keepdims=True)
        router_v[...] = prob * (onehot - gate_row)
        gate_all = jnp.transpose(jnp.broadcast_to(gate_row, (128, n_tok)))
        gate_v[...] = gate_all
        gate = gate_all[:, :1]
        load_gy.wait()
        dispatch(1, (gate * gy_v[...].astype(F32)).astype(BF16))

    def meet():
        @pl.when(at_end)
        def _():
            pl.semaphore_wait(barrier, 7)

        @pl.when(jnp.logical_not(at_end))
        def _():
            pl.semaphore_wait(barrier, 8)

    def step(name, f, *a):
        with jax.named_scope(name + "".join(str(v) for v in a if isinstance(v, int))):
            return f(*a)

    mask0, mask1 = pair_masks(rows, block, cap)

    OWN, MATE, NEAR, FAR, ALL = (j, 1), (near, 1), (side[0], 2), (side[1], 2), (0, N_EP)

    def group(ref, p, g):
        return ref[p, pl.ds(*g)].reshape(g[1] * block, ref.shape[-1])

    def put(ref, p, g, value):
        ref[p, pl.ds(*g)] = value.reshape(g[1], block, value.shape[-1])

    def wait_rows(t, p, far):
        wait_bytes(recv_v.at[t, p, pl.ds(0, 1 + far)], disp_recv.at[t, p, far])

    def one_dot(lhs, w_ref, p, which, dims=((1,), (0,))):
        mask = (mask0, mask1)[which]
        return dot(lhs * mask[: lhs.shape[0]], w_ref[2 * p + which], dims)

    def pair_dot(lhs, w_ref, p, *loads):
        terms = []
        for which in HALVES:
            if loads:
                loads[which].wait()
            terms.append(one_dot(lhs, w_ref, p, which))
        return terms[0] + terms[1]

    place = [z, N_TP - 1 - z]
    ahead, behind = [right, left], [left, right]

    cut = block // 16 * 8 + 8
    parts = [pl.ds(0, cut), pl.ds(cut, block - cut)]

    def rows_of(i, part):
        return parts[part] if i == LAST else slice(None)

    def rs_copy(i, h, q, part):
        where = rows_of(i, part)
        return remote(1, part_v.at[i, h, q, where], rs_in.at[i, h, q, where], rs_recv.at[i + part, h, q], tp=ahead[h])

    def rs_start(i, g, part):
        for h in HALVES:
            part_v[i, h, pl.ds(*g)] = part[:, h * half : (h + 1) * half].reshape(g[1], block, half)
        for h in HALVES:
            @pl.when(place[h] == 0)
            def _():
                for first, count in (NEAR, FAR) if g is ALL else (g,):
                    for b in range(count):
                        for n in HALVES if i == LAST else range(1):
                            rs_copy(i, h, first + b, n).start()

    def rs_relay(at, i, far, q, part):
        where = rows_of(i, part)
        for h in HALVES:
            @pl.when(place[h] == at)
            def _():
                rs_copy(i, h, q, part).wait_recv()
                part_v[i, h, q, where] = part_v[i, h, q, where] + rs_in[i, h, q, where]
                rs_copy(i, h, q, part).start()

    def hop_copy(i, h, q, far):
        return remote(2, red_v.at[i, q], slots_v.at[i, h, j], hop_recv.at[i, far], ep=q)

    def turn_copy(i, h, q, far):
        return remote(5, red_v.at[i, q], slots_v.at[i, h, j], turn_recv.at[i, far], tp=behind[h], ep=q)

    def last_turn(h, q, far):
        return remote(7, red_v.at[LAST, q], slots_v.at[LAST, h, j], last_recv.at[0, far, lax.rem(j, 2)], tp=behind[h], ep=q)

    def last_back(h, far, b):
        part = slots_v.at[LAST, h, side[far] + b]
        return remote(8, part, part, last_recv.at[1, far, b], tp=behind[h])

    def last_first(far, b):
        for h in HALVES:
            @pl.when(place[h] == 2)
            def _():
                wait_bytes(slots_v.at[LAST, h, 0], last_recv.at[0, far, b])
                last_back(h, far, b).start()

    def last_second(far, b):
        for h in HALVES:
            @pl.when(place[h] == 1)
            def _():
                last_back(h, far, b).wait_recv()
                last_back(h, far, b).start()

    def last_last(far, b):
        for h in HALVES:
            @pl.when(place[h] == 0)
            def _():
                last_back(h, far, b).wait_recv()

    def rs_final(i, far, q, part):
        where = rows_of(i, part)
        for h in HALVES:
            @pl.when(place[h] == N_TP - 1)
            def _():
                rs_copy(i, h, q, part).wait_recv()
                red_v[i, q, where] = (part_v[i, h, q, where] + rs_in[i, h, q, where]).astype(BF16)
                if i == LAST and part == 0:
                    return
                if i == LAST:
                    last_turn(h, q, far).start()
                else:
                    turn_copy(i, h, q, far).start()
                if far:
                    hop_copy(i, h, q, far).start()
                else:
                    @pl.when(j != q)
                    def _():
                        hop_copy(i, h, q, far).start()

                    @pl.when(j == q)
                    def _():
                        slots_v[i, h, j] = red_v[i, q]

    def hop_wait(i):
        for far in HALVES:
            wait_bytes(slots_v.at[i, 0, pl.ds(0, 1 + far)], hop_recv.at[i, far])

    def hop_wait_end(i):
        @pl.when(at_end)
        def _():
            hop_wait(i)

    def back_copy(i, h, far):
        part = slots_v.at[i, h, pl.ds(side[far], 2)]
        return remote(3, part, part, back_recv.at[i, far], tp=behind[h])

    def back_first(i, far):
        for h in HALVES:
            @pl.when(place[h] == 2)
            def _():
                wait_bytes(slots_v.at[i, h, pl.ds(0, 2)], turn_recv.at[i, far])
                back_copy(i, h, far).start()

    def back_second(i, far):
        for h in HALVES:
            @pl.when(place[h] == 1)
            def _():
                back_copy(i, h, far).wait_recv()
                back_copy(i, h, far).start()

    def back_last(i, far):
        for h in HALVES:
            @pl.when(place[h] == 0)
            def _():
                back_copy(i, h, far).wait_recv()

    def gate_copy(h, at):
        tp = at if h == 0 else N_TP - 1 - at
        return remote(10, gate_rows.at[h], gate_rows.at[h], gate_recv.at[h], tp=tp)

    def gate_root():
        for h in HALVES:
            @pl.when(place[h] == N_TP - 1)
            def _():
                hop_wait(0)
                hop_wait(1)
                y_tok = half_by_token(onehot_slots, slots_v, 0, h)
                part = jnp.sum(gy_v[:, h * half : (h + 1) * half].astype(F32) * y_tok, axis=1, keepdims=True)
                gate_rows[h] = jnp.transpose(jnp.broadcast_to(part, (n_tok, 128)))[:8]
                for at in range(N_TP - 1):
                    gate_copy(h, at).start()

    def wg_copy(k):
        return remote(4, dwg_part, dwg_in.at[k], wg_recv, ep=ep_peer[k])

    def router_back():
        for h in HALVES:
            @pl.when(place[h] != N_TP - 1)
            def _():
                gate_copy(h, 0).wait_recv()
        d_logits = (gate_rows[0, :1] + gate_rows[1, :1]) * router_v[...]
        dwg_part[...] = dot(d_logits.astype(BF16), x_v[...])
        for k in range(3):
            wg_copy(k).start()
        rgrad_v[...] = dot(jnp.transpose(d_logits).astype(BF16), wg_ref[...])

    def forward_act(p, g, *loads):
        a = pair_dot(group(recv_v.at[0], p, g), wi_v, p, *loads)
        put(act_v, p, g, a)
        put(h_v, p, g, (0.5 * a * (1.0 + jnp.tanh(GELU_C * (a + GELU_K * a * a * a)))).astype(BF16))

    def forward_out(p, g, *loads):
        rs_start(p, g, pair_dot(group(h_v, p, g), wo_v, p, *loads))

    NT = ((1,), (1,))

    def backward_act0(p, g):
        put(tmp_v, 0, g, one_dot(group(recv_v.at[1], p, g), wo_v, p, 0, NT))

    def backward_act1(p, g):
        dh = group(tmp_v, 0, g) + one_dot(group(recv_v.at[1], p, g), wo_v, p, 1, NT)
        a = group(act_v, p, g)
        a2 = a * a
        th = jnp.tanh(GELU_C * (a + GELU_K * a2 * a))
        slope = 0.5 * (1.0 + th) + 0.5 * a * (1.0 - th * th) * (GELU_C * (1.0 + 3.0 * GELU_K * a2))
        put(da_v, p, g, (dh * slope).astype(BF16))

    def backward_in0(p, g):
        put(tmp_v, 1, g, one_dot(group(da_v, p, g), wi_v, p, 0, NT))

    def backward_in1(p, g):
        rs_start(2 + p, g, group(tmp_v, 1, g) + one_dot(group(da_v, p, g), wi_v, p, 1, NT))

    def weight_grad(n):
        e = n // 2
        p, mask = e // 2, (mask0, mask1)[e % 2]
        if n % 2 == 0:
            dwo_v[e] = dot(group(h_v, p, ALL) * mask, group(recv_v.at[1], p, ALL), ((0,), (0,)))
        else:
            dwi_v[e] = dot(group(recv_v.at[0], p, ALL) * mask, group(da_v, p, ALL), ((0,), (0,)))

    order = [(0, 0, OWN), (0, 0, MATE), (1, 0, NEAR), (2, 0, NEAR), (0, 1, FAR), (1, 1, FAR), (2, 1, FAR), (3, 0, NEAR), (3, 1, FAR)]
    chunks = [(i, far, g[0] + b, n) for i, far, g in order for b in range(g[1]) for n in (HALVES if i == LAST else range(1))]

    pieces = [(0, 0), (1, 0), (2, 0), (0, 1), (1, 1), (2, 1)]

    def relay(at, k):
        with jax.named_scope(f"relay{at}_{k}"):
            if at == 3:
                back_first(*pieces[k])
            else:
                rs_relay(at, *chunks[k])

    def wait_both(t, p):
        wait_rows(t, p, 0)
        wait_rows(t, p, 1)

    def own_act():
        forward_act(0, OWN, *load_wi[:2])

    def own_out():
        forward_out(0, OWN, *load_wo[:2])

    def start_mate():
        wait_rows(0, 0, 0)
        forward_act(0, MATE)
        forward_out(0, MATE)

    def near_next():
        load_wi[2].wait()
        wait_rows(0, 1, 0)
        forward_act(1, NEAR)

    def near_next_out():
        load_wo[2].wait()
        forward_out(1, NEAR)

    def back_units(p, g, wait):
        def head():
            wait()
            backward_act0(p, g)

        return [head] + [functools.partial(f, p, g) for f in (backward_act1, backward_in0, backward_in1)]

    def far_units(p):
        def head():
            wait_rows(0, p, 1)
            forward_act(p, FAR)

        return [head, functools.partial(forward_out, p, FAR)]

    step("route_x", route_x)
    step("meet", meet)
    start_dispatch(0)
    step("own_act", own_act)
    step("own_out", own_out)
    step("mate", start_mate)
    step("route_dy", route_dy)
    keep_own(1)
    start_dispatch(1)
    step("near1", near_next)
    step("near1_out", near_next_out)

    def timed(ready, lengths, units):
        return [(ready, length, f) for length, f in zip(lengths, units)]

    work = timed(7.0, (0.42, 0.62, 0.42, 0.62), back_units(0, NEAR, lambda: wait_rows(1, 0, 0)))
    work += timed(7.9, (0.62, 0.62), far_units(0)) + timed(11.0, (0.62, 0.62), far_units(1))
    work += timed(13.5, (0.42, 0.6, 0.42, 0.6), back_units(0, FAR, lambda: wait_rows(1, 0, 1)))
    work += timed(16.5, (0.47, 0.65, 0.47, 0.65), back_units(1, ALL, lambda: wait_both(1, 1)))
    work += timed(16.5, (0.61,) * 8, [functools.partial(weight_grad, n) for n in range(8)])
    when = [1.33 * (min(k, 12) + max(k - 12, 0) / 2) for k in range(20)]
    relays = [(start + t, at, k) for start, at in ((7.0, 1), (11.4, 2)) for k, t in enumerate(when)]
    relays = sorted(relays + [(28.4 + 1.31 * k, 3, k) for k in range(3)])
    now, n_work = 7.2, 0
    while relays or work:
        due = relays[0][0] if relays else 1e9
        ready = work[0][0] if work else 1e9
        if work and ready <= now and (now + work[0][1] <= due + 0.15):
            step(f"work{n_work}", work[0][2])
            now += work.pop(0)[1]
            n_work += 1
        elif relays and due <= max(now, ready):
            relay(*relays.pop(0)[1:])
            now = max(now, due) + 0.1
        else:
            now = min(due, max(now, ready)) if ready > now else due

    def turn(i, far):
        step("back1_", back_first, i, far)

    def back(i, far):
        step("back2_", back_second, i, far)

    for k, chunk in enumerate(chunks):
        step(f"final{k}", lambda: rs_final(*chunk))
        if k == 12:
            step("gate_root", gate_root)
    def finish_wg():
        wait_bytes(dwg_in, wg_recv)
        dwg_v[...] = (dwg_part[...] + dwg_in[0]) + (dwg_in[1] + dwg_in[2])

    def hand_over():
        back_v[...] = slots_v[...]

    blocks = [(far, b) for far in HALVES for b in HALVES]
    for n in range(2, 6):
        if n > 2:
            turn(*pieces[n])
        back(*pieces[n - 2])
    step("router_back", router_back)
    back(*pieces[4])
    step("last_first", last_first, *blocks[0])
    step("last_first", last_first, *blocks[1])
    back(*pieces[5])
    step("last_first", last_first, *blocks[2])
    step("last_first", last_first, *blocks[3])
    for far, b in blocks:
        step("last_second", last_second, far, b)
    for piece in pieces:
        step("back3_", back_last, *piece)
    for far, b in blocks:
        step("last_last", last_last, far, b)
    step("hop_", hop_wait_end, 2)
    step("hop_", hop_wait_end, 3)
    step("hand_over", hand_over)
    step("finish_wg", finish_wg)

    def drain():
        wait_bytes(part_v.at[pl.ds(0, N_EP - 1), 0], sent_sem.at[0])
        wait_bytes(dwg_in, sent_sem.at[4])

        @pl.when(at_end)
        def _():
            wait_bytes(part_v.at[:, 0], sent_sem.at[1])
            wait_bytes(red_v.at[:, pl.ds(0, N_EP - 1)], sent_sem.at[2])
            wait_bytes(red_v.at[pl.ds(0, 3)], sent_sem.at[5])
            wait_bytes(red_v.at[0], sent_sem.at[7])
            wait_bytes(gate_rows.at[pl.ds(0, 3)], sent_sem.at[10])

        @pl.when(jnp.logical_not(at_end))
        def _():
            wait_bytes(part_v, sent_sem.at[1])
            wait_bytes(slots_v.at[pl.ds(0, 3)], sent_sem.at[3])
            wait_bytes(slots_v.at[0], sent_sem.at[8])

    step("drain", drain)


def store_kernel(
    gate_v, back_v, onehot_slots, rgrad_v, dwg_v, dwi_v, dwo_v, out_hbm, dx_hbm, dwg_hbm, dwi_hbm, dwo_hbm, out_v, dx_v, sem
):
    pairs = [(dwi_v.at[e], dwi_hbm.at[e]) for e in range(4)] + [(dwo_v.at[e], dwo_hbm.at[e]) for e in range(4)]
    pairs += [(dwg_v, dwg_hbm), (out_v, out_hbm), (dx_v, dx_hbm)]
    copies = [pltpu.make_async_copy(src, dst, sem.at[n]) for n, (src, dst) in enumerate(pairs)]
    for cp in copies[:-2]:
        cp.start()
    out_v[...] = (gate_v[:, :1] * by_token(onehot_slots, back_v, 0)).astype(BF16)
    copies[-2].start()
    dx_v[...] = (by_token(onehot_slots, back_v, 2) + rgrad_v[...]).astype(BF16)
    copies[-1].start()
    for cp in copies:
        cp.wait()


def solution(mesh):
    row_spec = P(("dp", "ep"), None)

    def local_block(tokens, grad_out, w_router, w_in, w_out, expert_ids):
        n_tok, d_model = tokens.shape
        n_exp = w_router.shape[1]
        n_loc, _, f_loc = w_in.shape
        cap = (6 * n_tok + 5 * n_exp - 1) // (5 * n_exp)
        block, rows, half = 2 * cap, 8 * cap, d_model // 2
        S = jax.ShapeDtypeStruct
        any_spec, vmem_spec = pl.BlockSpec(memory_space=pl.ANY), pl.BlockSpec(memory_space=pltpu.VMEM)
        dma = pltpu.SemaphoreType.DMA
        out_shape = (
            S((n_tok, d_model), BF16), S((n_tok, d_model), BF16), S((n_exp, d_model), F32),
            S((n_loc, d_model, f_loc), F32), S((n_loc, f_loc, d_model), F32),
        )
        handed = (
            S((n_tok, 128), F32), S((4, 2, N_EP, block, half), BF16), S((2 * rows, n_tok), BF16), S((n_tok, d_model), F32),
        ) + out_shape[2:]
        held = tuple(pltpu.VMEM(s.shape, s.dtype) for s in handed)
        scratch = [
            pltpu.VMEM((1, n_tok), jnp.int32), pltpu.VMEM((n_exp, d_model), BF16),
            pltpu.VMEM((n_tok, d_model), BF16), pltpu.VMEM((n_tok, d_model), BF16),
            pltpu.VMEM(w_in.shape, BF16), pltpu.VMEM(w_out.shape, BF16),
            pltpu.VMEM((n_exp, n_tok), F32),
            pltpu.VMEM((2, 2, N_EP, block, d_model), BF16), pltpu.VMEM((2, 2, N_EP, block, d_model), BF16),
            pltpu.VMEM((2, N_EP, block, f_loc), F32), pltpu.VMEM((2, N_EP, block, f_loc), BF16),
            pltpu.VMEM((2, N_EP, block, f_loc), BF16), pltpu.VMEM((2, N_EP, block, d_model), F32),
            pltpu.VMEM((4, 2, N_EP, block, half), F32), pltpu.VMEM((4, 2, N_EP, block, half), F32),
            pltpu.VMEM((4, N_EP, block, half), BF16), pltpu.VMEM((4, 2, N_EP, block, half), BF16),
            pltpu.VMEM((n_exp, d_model), F32), pltpu.VMEM((3, n_exp, d_model), F32), pltpu.VMEM((4, 8, n_tok), F32),
            dma((10,)), dma((11,)), dma((2, 2, 2)), dma((5, 2, N_EP)), dma((4, 2)), dma((3, 2)), dma((3, 2)), dma((2, 2, 2)), dma, dma((2,)),
        ]
        results = pl.pallas_call(
            functools.partial(moe_kernel, cap),
            out_shape=held,
            in_specs=[any_spec] * 6,
            out_specs=(vmem_spec,) * 7,
            scratch_shapes=scratch,
            compiler_params=pltpu.CompilerParams(collective_id=0, has_side_effects=True, vmem_limit_bytes=24 * 2**20),
        )(*[
            pltpu.with_memory_space_constraint(r, pltpu.HBM)
            for r in (expert_ids.reshape(1, n_tok), w_router.T, tokens, grad_out, w_in, w_out)
        ])
        out, dx, dwg, dwi, dwo = pl.pallas_call(
            store_kernel,
            out_shape=out_shape,
            in_specs=[vmem_spec] * 7,
            out_specs=(any_spec,) * 5,
            scratch_shapes=[pltpu.VMEM((n_tok, d_model), BF16), pltpu.VMEM((n_tok, d_model), BF16), dma((11,))],
            compiler_params=pltpu.CompilerParams(vmem_limit_bytes=8 * 2**20),
        )(*[pltpu.with_memory_space_constraint(r, pltpu.VMEM) for r in results])
        return out, dx, dwi, dwo, dwg.T

    in_specs = (row_spec, row_spec, P(None, None), P("ep", None, "tp"), P("ep", "tp", None), P(("dp", "ep")))
    out_specs = (row_spec, row_spec, P(("dp", "ep"), None, "tp"), P(("dp", "ep"), "tp", None), P("dp", None))
    return jax.shard_map(local_block, mesh=mesh, in_specs=in_specs, out_specs=out_specs, check_vma=False)
```

```python
import functools

import jax
import jax.numpy as jnp
from jax import lax
from jax.experimental import pallas as pl
from jax.experimental.pallas import tpu as pltpu
from jax.sharding import PartitionSpec as P

MESH = pl.DeviceIdType.MESH
F32, BF16 = jnp.float32, jnp.bfloat16
GELU_C = 0.7978845608028654
GELU_K = 0.044715
N_EP, N_TP, N_PAIR = 4, 4, 2
HALVES = range(2)
LAST = 3


def dot(a, b, dims=((1,), (0,))):
    return lax.dot_general(a, b, (dims, ((), ())), preferred_element_type=F32)


def pair_masks(rows, block, cap):
    row = lax.broadcasted_iota(jnp.int32, (rows, 1), 0)
    first = lax.rem(row, block) < cap
    return jnp.where(first, 1.0, 0.0).astype(BF16), jnp.where(first, 0.0, 1.0).astype(BF16)


def half_by_token(onehot_slots, slots, first, h):
    n, width = onehot_slots.shape[0] // 2, slots.shape[-1]
    return dot(onehot_slots[...], jnp.concatenate([slots[first + p, h].reshape(n, width) for p in range(2)], axis=0), ((0,), (0,)))


def by_token(onehot_slots, slots, first):
    n, width = onehot_slots.shape[0] // 2, slots.shape[-1]
    halves = [jnp.concatenate([slots[first + p, h].reshape(n, width) for p in range(2)], axis=0) for h in HALVES]
    return dot(onehot_slots[...], jnp.concatenate(halves, axis=1), ((0,), (0,)))


def moe_kernel(
    cap,
    ids_hbm, wg_hbm, x_hbm, gy_hbm, wi_hbm, wo_hbm,
    gate_v, slots_v, onehot_slots, rgrad_v, dwg_v, dwi_v, dwo_v,
    ids_ref, wg_ref, x_v, gy_v, wi_v, wo_v,
    router_v, send_v, recv_v, act_v, h_v, da_v, tmp_v,
    part_v, rs_in, red_v,
    dwg_part, dwg_in, gate_rows,
    load_sem, sent_sem, disp_recv, rs_recv, hop_recv, back_recv, last_recv, wg_recv, gate_recv,
):
    block = 2 * cap
    rows = N_EP * block
    n_tok, d_model = x_v.shape
    n_exp = wg_ref.shape[0]
    half = d_model // 2
    z, j = lax.axis_index("tp"), lax.axis_index("ep")
    right, left = lax.rem(z + 1, N_TP), lax.rem(z + N_TP - 1, N_TP)
    chip = j // 2
    near = j + 1 - 2 * lax.rem(j, 2)
    ep_peer = [near, lax.rem(j + 2, N_EP), lax.rem(near + 2, N_EP)]
    side = [2 * chip, 2 - 2 * chip]

    def remote(kind, src, dst, rsem, **dev):
        return pltpu.make_async_remote_copy(
            src_ref=src, dst_ref=dst, send_sem=sent_sem.at[kind], recv_sem=rsem, device_id=dev, device_id_type=MESH
        )

    def wait_bytes(ref, sem):
        pltpu.make_async_copy(ref, ref, sem).wait()

    load_x = pltpu.make_async_copy(x_hbm, x_v, load_sem.at[0])
    load_gy = pltpu.make_async_copy(gy_hbm, gy_v, load_sem.at[1])
    def load_weights(src, dst, first, count, n):
        return pltpu.make_async_copy(src.at[pl.ds(first, count)], dst.at[pl.ds(first, count)], load_sem.at[n])

    load_wi = [load_weights(wi_hbm, wi_v, *a) for a in ((0, 1, 2), (1, 1, 3), (2, 2, 4))]
    load_wo = [load_weights(wo_hbm, wo_v, *a) for a in ((0, 1, 8), (1, 1, 9), (2, 2, 5))]
    load_ids = pltpu.make_async_copy(ids_hbm, ids_ref, load_sem.at[6])
    load_wg = pltpu.make_async_copy(wg_hbm, wg_ref, load_sem.at[7])
    for load in (load_ids, load_x, *load_wi[:2], *load_wo[:2], load_wg, load_gy, load_wi[2], load_wo[2]):
        load.start()

    barrier = pltpu.get_barrier_semaphore()
    pair_z = z + 1 - 2 * lax.rem(z, 2)
    at_end = (z == 0) | (z == N_TP - 1)

    def greet(**dev):
        pl.semaphore_signal(barrier, inc=1, device_id=dev, device_id_type=MESH)

    for peer in ep_peer:
        greet(ep=peer)
    for peer in [j] + ep_peer:
        greet(tp=pair_z, ep=peer)

    @pl.when(jnp.logical_not(at_end))
    def _():
        greet(tp=N_TP - 1 - z)

    load_ids.wait()
    ids = ids_ref[...]
    chosen = ids == lax.broadcasted_iota(jnp.int32, (n_exp, n_tok), 0)
    onehot = jnp.where(chosen, 1.0, 0.0)
    before = lax.broadcasted_iota(jnp.int32, (n_tok, n_tok), 0) < lax.broadcasted_iota(jnp.int32, (n_tok, n_tok), 1)
    counts = dot(onehot.astype(BF16), jnp.where(before, 1.0, 0.0).astype(BF16))
    pos = jnp.sum(counts * onehot, axis=0, keepdims=True)
    base = ((ids >> 1) & 1) * rows + (ids >> 2) * block + (ids & 1) * cap
    slot = jnp.where(pos < cap, base.astype(F32) + pos, -1.0)
    slot_iota = lax.broadcasted_iota(jnp.int32, (2 * rows, n_tok), 0).astype(F32)
    onehot_slots[...] = jnp.where(slot_iota == slot, 1.0, 0.0).astype(BF16)

    def dispatch(t, tok_rows):
        packed = dot(onehot_slots[...], tok_rows).astype(BF16)
        send_v[t] = packed.reshape(2, N_EP, block, d_model)

    def disp_copy(t, p, k):
        peer = ep_peer[k]
        return remote(0, send_v.at[t, p, peer], recv_v.at[t, p, j], disp_recv.at[t, p, min(k, 1)], ep=peer)

    def start_dispatch(t):
        for p in range(N_PAIR):
            disp_copy(t, p, 0).start()
        for p in range(N_PAIR):
            for k in (1, 2):
                disp_copy(t, p, k).start()

    def keep_own(t):
        for p in range(N_PAIR):
            recv_v[t, p, j] = send_v[t, p, j]

    def route_x():
        load_x.wait()
        dispatch(0, x_v[...])
        keep_own(0)

    def route_dy():
        load_wg.wait()
        logits = dot(wg_ref[...], x_v[...], ((1,), (1,)))
        expd = jnp.exp(logits - jnp.max(logits, axis=0, keepdims=True))
        prob = expd / jnp.sum(expd, axis=0, keepdims=True)
        gate_row = jnp.sum(jnp.where(chosen, prob, 0.0), axis=0, keepdims=True)
        router_v[...] = prob * (onehot - gate_row)
        gate_all = jnp.transpose(jnp.broadcast_to(gate_row, (128, n_tok)))
        gate_v[...] = gate_all
        gate = gate_all[:, :1]
        load_gy.wait()
        dispatch(1, (gate * gy_v[...].astype(F32)).astype(BF16))

    def meet():
        @pl.when(at_end)
        def _():
            pl.semaphore_wait(barrier, 7)

        @pl.when(jnp.logical_not(at_end))
        def _():
            pl.semaphore_wait(barrier, 8)

    def step(name, f, *a):
        with jax.named_scope(name + "".join(str(v) for v in a if isinstance(v, int))):
            return f(*a)

    mask0, mask1 = pair_masks(rows, block, cap)

    OWN, MATE, NEAR, FAR, ALL = (j, 1), (near, 1), (side[0], 2), (side[1], 2), (0, N_EP)

    def group(ref, p, g):
        return ref[p, pl.ds(*g)].reshape(g[1] * block, ref.shape[-1])

    def put(ref, p, g, value):
        ref[p, pl.ds(*g)] = value.reshape(g[1], block, value.shape[-1])

    def wait_rows(t, p, far):
        wait_bytes(recv_v.at[t, p, pl.ds(0, 1 + far)], disp_recv.at[t, p, far])

    def one_dot(lhs, w_ref, p, which, dims=((1,), (0,))):
        mask = (mask0, mask1)[which]
        return dot(lhs * mask[: lhs.shape[0]], w_ref[2 * p + which], dims)

    def pair_dot(lhs, w_ref, p, *loads):
        terms = []
        for which in HALVES:
            if loads:
                loads[which].wait()
            terms.append(one_dot(lhs, w_ref, p, which))
        return terms[0] + terms[1]

    place = [z, N_TP - 1 - z]
    ahead, behind = [right, left], [left, right]

    cut = block // 16 * 8 + 8
    parts = [pl.ds(0, cut), pl.ds(cut, block - cut)]

    def rows_of(i, part):
        return parts[part] if i == LAST else slice(None)

    def rs_copy(i, h, q, part):
        where = rows_of(i, part)
        return remote(1, part_v.at[i, h, q, where], rs_in.at[i, h, q, where], rs_recv.at[i + part, h, q], tp=ahead[h])

    def rs_start(i, g, part):
        for h in HALVES:
            part_v[i, h, pl.ds(*g)] = part[:, h * half : (h + 1) * half].reshape(g[1], block, half)
        for h in HALVES:
            @pl.when(place[h] == 0)
            def _():
                for first, count in (NEAR, FAR) if g is ALL else (g,):
                    for b in range(count):
                        for n in HALVES if i == LAST else range(1):
                            rs_copy(i, h, first + b, n).start()

    def rs_relay(at, i, far, q, part):
        where = rows_of(i, part)
        for h in HALVES:
            @pl.when(place[h] == at)
            def _():
                rs_copy(i, h, q, part).wait_recv()
                part_v[i, h, q, where] = part_v[i, h, q, where] + rs_in[i, h, q, where]
                rs_copy(i, h, q, part).start()

    def hop_copy(i, h, q, far):
        return remote(2, red_v.at[i, q], slots_v.at[i, h, j], hop_recv.at[i, far], ep=q)

    def turn_copy(i, h, q, far):
        return remote(5, red_v.at[i, q], slots_v.at[i, h, j], hop_recv.at[i, far], tp=behind[h], ep=q)

    def last_turn(h, q, far):
        return remote(7, red_v.at[LAST, q], slots_v.at[LAST, h, j], last_recv.at[0, far, lax.rem(j, 2)], tp=behind[h], ep=q)

    def last_back(h, far, b):
        part = slots_v.at[LAST, h, side[far] + b]
        return remote(8, part, part, last_recv.at[1, far, b], tp=behind[h])

    def last_first(far, b):
        for h in HALVES:
            @pl.when(place[h] == 2)
            def _():
                wait_bytes(slots_v.at[LAST, h, 0], last_recv.at[0, far, b])
                last_back(h, far, b).start()

    def last_second(far, b):
        for h in HALVES:
            @pl.when(place[h] == 1)
            def _():
                last_back(h, far, b).wait_recv()
                last_back(h, far, b).start()

    def last_last(far, b):
        for h in HALVES:
            @pl.when(place[h] == 0)
            def _():
                last_back(h, far, b).wait_recv()

    def rs_final(i, far, q, part):
        where = rows_of(i, part)
        for h in HALVES:
            @pl.when(place[h] == N_TP - 1)
            def _():
                rs_copy(i, h, q, part).wait_recv()
                red_v[i, q, where] = (part_v[i, h, q, where] + rs_in[i, h, q, where]).astype(BF16)
                if i == LAST and part == 0:
                    return
                if i == LAST:
                    last_turn(h, q, far).start()
                else:
                    turn_copy(i, h, q, far).start()
                if far:
                    hop_copy(i, h, q, far).start()
                else:
                    @pl.when(j != q)
                    def _():
                        hop_copy(i, h, q, far).start()

                    @pl.when(j == q)
                    def _():
                        slots_v[i, h, j] = red_v[i, q]

    def hop_wait(i):
        for far in HALVES:
            wait_bytes(slots_v.at[i, 0, pl.ds(0, 1 + far)], hop_recv.at[i, far])

    def hop_wait_end(i):
        @pl.when(at_end)
        def _():
            hop_wait(i)

    def back_copy(i, h, far):
        part = slots_v.at[i, h, pl.ds(side[far], 2)]
        return remote(3, part, part, back_recv.at[i, far], tp=behind[h])

    def back_first(i, far):
        for h in HALVES:
            @pl.when(place[h] == 2)
            def _():
                wait_bytes(slots_v.at[i, h, pl.ds(0, 2)], hop_recv.at[i, far])
                back_copy(i, h, far).start()

    def back_second(i, far):
        for h in HALVES:
            @pl.when(place[h] == 1)
            def _():
                back_copy(i, h, far).wait_recv()
                back_copy(i, h, far).start()

    def back_last(i, far):
        for h in HALVES:
            @pl.when(place[h] == 0)
            def _():
                back_copy(i, h, far).wait_recv()

    def gate_copy(h, at):
        tp = at if h == 0 else N_TP - 1 - at
        return remote(6, gate_rows.at[h], gate_rows.at[h], gate_recv.at[h], tp=tp)

    def gate_root():
        for h in HALVES:
            @pl.when(place[h] == N_TP - 1)
            def _():
                hop_wait(0)
                hop_wait(1)
                y_tok = half_by_token(onehot_slots, slots_v, 0, h)
                part = jnp.sum(gy_v[:, h * half : (h + 1) * half].astype(F32) * y_tok, axis=1, keepdims=True)
                gate_rows[h] = jnp.transpose(jnp.broadcast_to(part, (n_tok, 128)))[:8]
                for at in range(N_TP - 1):
                    gate_copy(h, at).start()

    def wg_copy(k):
        return remote(4, dwg_part, dwg_in.at[k], wg_recv, ep=ep_peer[k])

    def router_back():
        for h in HALVES:
            @pl.when(place[h] != N_TP - 1)
            def _():
                gate_copy(h, 0).wait_recv()
        d_logits = (gate_rows[0, :1] + gate_rows[1, :1]) * router_v[...]
        dwg_part[...] = dot(d_logits.astype(BF16), x_v[...])
        for k in range(3):
            wg_copy(k).start()
        rgrad_v[...] = dot(jnp.transpose(d_logits).astype(BF16), wg_ref[...])

    def forward_act(p, g, *loads):
        a = pair_dot(group(recv_v.at[0], p, g), wi_v, p, *loads)
        put(act_v, p, g, a)
        put(h_v, p, g, (0.5 * a * (1.0 + jnp.tanh(GELU_C * (a + GELU_K * a * a * a)))).astype(BF16))

    def forward_out(p, g, *loads):
        rs_start(p, g, pair_dot(group(h_v, p, g), wo_v, p, *loads))

    NT = ((1,), (1,))

    def backward_act0(p, g):
        put(tmp_v, 0, g, one_dot(group(recv_v.at[1], p, g), wo_v, p, 0, NT))

    def backward_act1(p, g):
        dh = group(tmp_v, 0, g) + one_dot(group(recv_v.at[1], p, g), wo_v, p, 1, NT)
        a = group(act_v, p, g)
        a2 = a * a
        th = jnp.tanh(GELU_C * (a + GELU_K * a2 * a))
        slope = 0.5 * (1.0 + th) + 0.5 * a * (1.0 - th * th) * (GELU_C * (1.0 + 3.0 * GELU_K * a2))
        put(da_v, p, g, (dh * slope).astype(BF16))

    def backward_in0(p, g):
        put(tmp_v, 1, g, one_dot(group(da_v, p, g), wi_v, p, 0, NT))

    def backward_in1(p, g):
        rs_start(2 + p, g, group(tmp_v, 1, g) + one_dot(group(da_v, p, g), wi_v, p, 1, NT))

    def weight_grad(n):
        e = n // 2
        p, mask = e // 2, (mask0, mask1)[e % 2]
        if n % 2 == 0:
            dwo_v[e] = dot(group(h_v, p, ALL) * mask, group(recv_v.at[1], p, ALL), ((0,), (0,)))
        else:
            dwi_v[e] = dot(group(recv_v.at[0], p, ALL) * mask, group(da_v, p, ALL), ((0,), (0,)))

    order = [(0, 0, OWN), (0, 0, MATE), (1, 0, NEAR), (2, 0, NEAR), (0, 1, FAR), (1, 1, FAR), (2, 1, FAR), (3, 0, NEAR), (3, 1, FAR)]
    chunks = [(i, far, g[0] + b, n) for i, far, g in order for b in range(g[1]) for n in (HALVES if i == LAST else range(1))]

    pieces = [(0, 0), (1, 0), (2, 0), (0, 1), (1, 1), (2, 1)]

    def relay(at, k):
        with jax.named_scope(f"relay{at}_{k}"):
            if at == 3:
                back_first(*pieces[k])
            else:
                rs_relay(at, *chunks[k])

    def wait_both(t, p):
        wait_rows(t, p, 0)
        wait_rows(t, p, 1)

    def own_act():
        forward_act(0, OWN, *load_wi[:2])

    def own_out():
        forward_out(0, OWN, *load_wo[:2])

    def start_mate():
        wait_rows(0, 0, 0)
        forward_act(0, MATE)
        forward_out(0, MATE)

    def near_next():
        load_wi[2].wait()
        wait_rows(0, 1, 0)
        forward_act(1, NEAR)

    def near_next_out():
        load_wo[2].wait()
        forward_out(1, NEAR)

    def back_units(p, g, wait):
        def head():
            wait()
            backward_act0(p, g)

        return [head] + [functools.partial(f, p, g) for f in (backward_act1, backward_in0, backward_in1)]

    def far_units(p):
        def head():
            wait_rows(0, p, 1)
            forward_act(p, FAR)

        return [head, functools.partial(forward_out, p, FAR)]

    step("route_x", route_x)
    step("meet", meet)
    start_dispatch(0)
    step("own_act", own_act)
    step("own_out", own_out)
    step("mate", start_mate)
    step("route_dy", route_dy)
    keep_own(1)
    start_dispatch(1)
    step("near1", near_next)
    step("near1_out", near_next_out)

    def timed(ready, lengths, units):
        return [(ready, length, f) for length, f in zip(lengths, units)]

    work = timed(7.0, (0.42, 0.62, 0.42, 0.62), back_units(0, NEAR, lambda: wait_rows(1, 0, 0)))
    work += timed(7.9, (0.62, 0.62), far_units(0)) + timed(11.0, (0.62, 0.62), far_units(1))
    work += timed(13.5, (0.42, 0.6, 0.42, 0.6), back_units(0, FAR, lambda: wait_rows(1, 0, 1)))
    work += timed(16.5, (0.47, 0.65, 0.47, 0.65), back_units(1, ALL, lambda: wait_both(1, 1)))
    work += timed(16.5, (0.61,) * 8, [functools.partial(weight_grad, n) for n in range(8)])
    when = [1.33 * (min(k, 12) + max(k - 12, 0) / 2) for k in range(20)]
    relays = [(start + t, at, k) for start, at in ((7.0, 1), (11.4, 2)) for k, t in enumerate(when)]
    relays = sorted(relays + [(28.4 + 1.31 * k, 3, k) for k in range(3)])
    now, n_work = 7.2, 0
    while relays or work:
        due = relays[0][0] if relays else 1e9
        ready = work[0][0] if work else 1e9
        if work and ready <= now and (now + work[0][1] <= due + 0.15):
            step(f"work{n_work}", work[0][2])
            now += work.pop(0)[1]
            n_work += 1
        elif relays and due <= max(now, ready):
            relay(*relays.pop(0)[1:])
            now = max(now, due) + 0.1
        else:
            now = min(due, max(now, ready)) if ready > now else due

    def turn(i, far):
        step("back1_", back_first, i, far)

    def back(i, far):
        step("back2_", back_second, i, far)

    for k, chunk in enumerate(chunks):
        step(f"final{k}", lambda: rs_final(*chunk))
        if k == 12:
            step("gate_root", gate_root)
    def finish_wg():
        wait_bytes(dwg_in, wg_recv)
        dwg_v[...] = (dwg_part[...] + dwg_in[0]) + (dwg_in[1] + dwg_in[2])

    blocks = [(far, b) for far in HALVES for b in HALVES]
    for n in range(2, 6):
        if n > 2:
            turn(*pieces[n])
        back(*pieces[n - 2])
    step("router_back", router_back)
    back(*pieces[4])
    step("last_first", last_first, *blocks[0])
    step("last_first", last_first, *blocks[1])
    back(*pieces[5])
    step("last_first", last_first, *blocks[2])
    step("last_first", last_first, *blocks[3])
    for far, b in blocks:
        step("last_second", last_second, far, b)
    for piece in pieces:
        step("back3_", back_last, *piece)
    for far, b in blocks:
        step("last_last", last_last, far, b)
    step("hop_", hop_wait_end, 2)
    step("hop_", hop_wait_end, 3)
    step("finish_wg", finish_wg)

    def drain():
        wait_bytes(part_v.at[pl.ds(0, N_EP - 1), 0], sent_sem.at[0])
        wait_bytes(dwg_in, sent_sem.at[4])

        @pl.when(at_end)
        def _():
            wait_bytes(part_v.at[:, 0], sent_sem.at[1])
            wait_bytes(red_v.at[:, pl.ds(0, N_EP - 1)], sent_sem.at[2])
            wait_bytes(red_v.at[pl.ds(0, 3)], sent_sem.at[5])
            wait_bytes(red_v.at[0], sent_sem.at[7])
            wait_bytes(gate_rows.at[pl.ds(0, 3)], sent_sem.at[6])

        @pl.when(jnp.logical_not(at_end))
        def _():
            wait_bytes(part_v, sent_sem.at[1])
            wait_bytes(slots_v.at[pl.ds(0, 3)], sent_sem.at[3])
            wait_bytes(slots_v.at[0], sent_sem.at[8])

    step("drain", drain)


def store_kernel(
    gate_v, back_v, onehot_slots, rgrad_v, dwg_v, dwi_v, dwo_v, out_hbm, dx_hbm, dwg_hbm, dwi_hbm, dwo_hbm, out_v, dx_v, sem
):
    pairs = [(dwi_v.at[e], dwi_hbm.at[e]) for e in range(4)] + [(dwo_v.at[e], dwo_hbm.at[e]) for e in range(4)]
    pairs += [(dwg_v, dwg_hbm), (out_v, out_hbm), (dx_v, dx_hbm)]
    copies = [pltpu.make_async_copy(src, dst, sem.at[n]) for n, (src, dst) in enumerate(pairs)]
    for cp in copies[:-2]:
        cp.start()
    out_v[...] = (gate_v[:, :1] * by_token(onehot_slots, back_v, 0)).astype(BF16)
    copies[-2].start()
    dx_v[...] = (by_token(onehot_slots, back_v, 2) + rgrad_v[...]).astype(BF16)
    copies[-1].start()
    for cp in copies:
        cp.wait()


def solution(mesh):
    row_spec = P(("dp", "ep"), None)

    def local_block(tokens, grad_out, w_router, w_in, w_out, expert_ids):
        n_tok, d_model = tokens.shape
        n_exp = w_router.shape[1]
        n_loc, _, f_loc = w_in.shape
        cap = (6 * n_tok + 5 * n_exp - 1) // (5 * n_exp)
        block, rows, half = 2 * cap, 8 * cap, d_model // 2
        S = jax.ShapeDtypeStruct
        any_spec, vmem_spec = pl.BlockSpec(memory_space=pl.ANY), pl.BlockSpec(memory_space=pltpu.VMEM)
        dma = pltpu.SemaphoreType.DMA
        out_shape = (
            S((n_tok, d_model), BF16), S((n_tok, d_model), BF16), S((n_exp, d_model), F32),
            S((n_loc, d_model, f_loc), F32), S((n_loc, f_loc, d_model), F32),
        )
        handed = (
            S((n_tok, 128), F32), S((4, 2, N_EP, block, half), BF16), S((2 * rows, n_tok), BF16), S((n_tok, d_model), F32),
        ) + out_shape[2:]
        held = tuple(pltpu.VMEM(s.shape, s.dtype) for s in handed)
        scratch = [
            pltpu.VMEM((1, n_tok), jnp.int32), pltpu.VMEM((n_exp, d_model), BF16),
            pltpu.VMEM((n_tok, d_model), BF16), pltpu.VMEM((n_tok, d_model), BF16),
            pltpu.VMEM(w_in.shape, BF16), pltpu.VMEM(w_out.shape, BF16),
            pltpu.VMEM((n_exp, n_tok), F32),
            pltpu.VMEM((2, 2, N_EP, block, d_model), BF16), pltpu.VMEM((2, 2, N_EP, block, d_model), BF16),
            pltpu.VMEM((2, N_EP, block, f_loc), F32), pltpu.VMEM((2, N_EP, block, f_loc), BF16),
            pltpu.VMEM((2, N_EP, block, f_loc), BF16), pltpu.VMEM((2, N_EP, block, d_model), F32),
            pltpu.VMEM((4, 2, N_EP, block, half), F32), pltpu.VMEM((4, 2, N_EP, block, half), F32),
            pltpu.VMEM((4, N_EP, block, half), BF16),
            pltpu.VMEM((n_exp, d_model), F32), pltpu.VMEM((3, n_exp, d_model), F32), pltpu.VMEM((4, 8, n_tok), F32),
            dma((10,)), dma((9,)), dma((2, 2, 2)), dma((5, 2, N_EP)), dma((4, 2)), dma((3, 2)), dma((2, 2, 2)), dma, dma((2,)),
        ]
        results = pl.pallas_call(
            functools.partial(moe_kernel, cap),
            out_shape=held,
            in_specs=[any_spec] * 6,
            out_specs=(vmem_spec,) * 7,
            scratch_shapes=scratch,
            compiler_params=pltpu.CompilerParams(collective_id=0, has_side_effects=True, vmem_limit_bytes=24 * 2**20),
        )(*[
            pltpu.with_memory_space_constraint(r, pltpu.HBM)
            for r in (expert_ids.reshape(1, n_tok), w_router.T, tokens, grad_out, w_in, w_out)
        ])
        out, dx, dwg, dwi, dwo = pl.pallas_call(
            store_kernel,
            out_shape=out_shape,
            in_specs=[vmem_spec] * 7,
            out_specs=(any_spec,) * 5,
            scratch_shapes=[pltpu.VMEM((n_tok, d_model), BF16), pltpu.VMEM((n_tok, d_model), BF16), dma((11,))],
            compiler_params=pltpu.CompilerParams(vmem_limit_bytes=8 * 2**20),
        )(*[pltpu.with_memory_space_constraint(r, pltpu.VMEM) for r in results])
        return out, dx, dwi, dwo, dwg.T

    in_specs = (row_spec, row_spec, P(None, None), P("ep", None, "tp"), P("ep", "tp", None), P(("dp", "ep")))
    out_specs = (row_spec, row_spec, P(("dp", "ep"), None, "tp"), P(("dp", "ep"), "tp", None), P("dp", None))
    return jax.shard_map(local_block, mesh=mesh, in_specs=in_specs, out_specs=out_specs, check_vma=False)
```

```python
import functools

import jax
import jax.numpy as jnp
from jax import lax
from jax.experimental import pallas as pl
from jax.experimental.pallas import tpu as pltpu
from jax.sharding import PartitionSpec as P

MESH = pl.DeviceIdType.MESH
F32, BF16 = jnp.float32, jnp.bfloat16
GELU_C = 0.7978845608028654
GELU_K = 0.044715
N_EP, N_TP, N_PAIR = 4, 4, 2
HALVES = range(2)
LAST = 3


def dot(a, b, dims=((1,), (0,))):
    return lax.dot_general(a, b, (dims, ((), ())), preferred_element_type=F32)


def pair_masks(rows, block, cap):
    row = lax.broadcasted_iota(jnp.int32, (rows, 1), 0)
    first = lax.rem(row, block) < cap
    return jnp.where(first, 1.0, 0.0).astype(BF16), jnp.where(first, 0.0, 1.0).astype(BF16)


def half_by_token(onehot_slots, slots, first, h):
    n, width = onehot_slots.shape[0] // 2, slots.shape[-1]
    return dot(onehot_slots[...], jnp.concatenate([slots[first + p, h].reshape(n, width) for p in range(2)], axis=0), ((0,), (0,)))


def by_token(onehot_slots, slots, first):
    n, width = onehot_slots.shape[0] // 2, slots.shape[-1]
    halves = [jnp.concatenate([slots[first + p, h].reshape(n, width) for p in range(2)], axis=0) for h in HALVES]
    return dot(onehot_slots[...], jnp.concatenate(halves, axis=1), ((0,), (0,)))


def moe_kernel(
    cap,
    ids_hbm, wg_hbm, x_hbm, gy_hbm, wi_hbm, wo_hbm,
    gate_v, slots_v, onehot_slots, rgrad_v, dwg_v, dwi_v, dwo_v,
    ids_ref, wg_ref, x_v, gy_v, wi_v, wo_v,
    router_v, send_v, recv_v, act_v, h_v, da_v, tmp_v,
    part_v, rs_in, red_v,
    dwg_part, dwg_in, gate_rows,
    load_sem, sent_sem, disp_recv, rs_recv, hop_recv, last_recv, wg_recv, gate_recv,
):
    block = 2 * cap
    rows = N_EP * block
    n_tok, d_model = x_v.shape
    n_exp = wg_ref.shape[0]
    half = d_model // 2
    z, j = lax.axis_index("tp"), lax.axis_index("ep")
    right, left = lax.rem(z + 1, N_TP), lax.rem(z + N_TP - 1, N_TP)
    chip = j // 2
    near = j + 1 - 2 * lax.rem(j, 2)
    ep_peer = [near, lax.rem(j + 2, N_EP), lax.rem(near + 2, N_EP)]
    side = [2 * chip, 2 - 2 * chip]

    def remote(kind, src, dst, rsem, **dev):
        return pltpu.make_async_remote_copy(
            src_ref=src, dst_ref=dst, send_sem=sent_sem.at[kind], recv_sem=rsem, device_id=dev, device_id_type=MESH
        )

    def wait_bytes(ref, sem):
        pltpu.make_async_copy(ref, ref, sem).wait()

    load_x = pltpu.make_async_copy(x_hbm, x_v, load_sem.at[0])
    load_gy = pltpu.make_async_copy(gy_hbm, gy_v, load_sem.at[8])
    def load_weights(src, dst, first, count, n):
        return pltpu.make_async_copy(src.at[pl.ds(first, count)], dst.at[pl.ds(first, count)], load_sem.at[n])

    load_wi = [load_weights(wi_hbm, wi_v, *a) for a in ((0, 1, 2), (1, 1, 3), (2, 2, 6))]
    load_wo = [load_weights(wo_hbm, wo_v, *a) for a in ((0, 1, 4), (1, 1, 5), (2, 2, 7))]
    load_ids = pltpu.make_async_copy(ids_hbm, ids_ref, load_sem.at[1])
    load_wg = pltpu.make_async_copy(wg_hbm, wg_ref, load_sem.at[9])
    for load in (load_ids, load_x, *load_wi[:2], *load_wo[:2], load_wg, load_gy, load_wi[2], load_wo[2]):
        load.start()

    barrier = pltpu.get_barrier_semaphore()
    pair_z = z + 1 - 2 * lax.rem(z, 2)
    at_end = (z == 0) | (z == N_TP - 1)

    def greet(**dev):
        pl.semaphore_signal(barrier, inc=1, device_id=dev, device_id_type=MESH)

    for peer in ep_peer:
        greet(ep=peer)
    for peer in [j] + ep_peer:
        greet(tp=pair_z, ep=peer)

    @pl.when(jnp.logical_not(at_end))
    def _():
        greet(tp=N_TP - 1 - z)

    load_ids.wait()
    ids = ids_ref[...]
    chosen = ids == lax.broadcasted_iota(jnp.int32, (n_exp, n_tok), 0)
    onehot = jnp.where(chosen, 1.0, 0.0)
    before = lax.broadcasted_iota(jnp.int32, (n_tok, n_tok), 0) < lax.broadcasted_iota(jnp.int32, (n_tok, n_tok), 1)
    counts = dot(onehot.astype(BF16), jnp.where(before, 1.0, 0.0).astype(BF16))
    pos = jnp.sum(counts * onehot, axis=0, keepdims=True)
    base = ((ids >> 1) & 1) * rows + (ids >> 2) * block + (ids & 1) * cap
    slot = jnp.where(pos < cap, base.astype(F32) + pos, -1.0)
    slot_iota = lax.broadcasted_iota(jnp.int32, (2 * rows, n_tok), 0).astype(F32)
    onehot_slots[...] = jnp.where(slot_iota == slot, 1.0, 0.0).astype(BF16)

    def dispatch(t, tok_rows):
        packed = dot(onehot_slots[...], tok_rows).astype(BF16)
        send_v[t] = packed.reshape(2, N_EP, block, d_model)

    def disp_copy(t, p, k):
        peer = ep_peer[k]
        return remote(0, send_v.at[t, p, peer], recv_v.at[t, p, j], disp_recv.at[t, p, min(k, 1)], ep=peer)

    def start_dispatch(t):
        for p in range(N_PAIR):
            disp_copy(t, p, 0).start()
        for p in range(N_PAIR):
            for k in (1, 2):
                disp_copy(t, p, k).start()

    def keep_own(t):
        for p in range(N_PAIR):
            recv_v[t, p, j] = send_v[t, p, j]

    def route_x():
        load_x.wait()
        dispatch(0, x_v[...])
        keep_own(0)

    def route_dy():
        load_wg.wait()
        logits = dot(wg_ref[...], x_v[...], ((1,), (1,)))
        expd = jnp.exp(logits - jnp.max(logits, axis=0, keepdims=True))
        prob = expd / jnp.sum(expd, axis=0, keepdims=True)
        gate_row = jnp.sum(jnp.where(chosen, prob, 0.0), axis=0, keepdims=True)
        router_v[...] = prob * (onehot - gate_row)
        gate_all = jnp.transpose(jnp.broadcast_to(gate_row, (128, n_tok)))
        gate_v[...] = gate_all
        gate = gate_all[:, :1]
        load_gy.wait()
        dispatch(1, (gate * gy_v[...].astype(F32)).astype(BF16))

    def meet():
        @pl.when(at_end)
        def _():
            pl.semaphore_wait(barrier, 7)

        @pl.when(jnp.logical_not(at_end))
        def _():
            pl.semaphore_wait(barrier, 8)

    def step(name, f, *a):
        with jax.named_scope(name + "".join(str(v) for v in a if isinstance(v, int))):
            return f(*a)

    mask0, mask1 = pair_masks(rows, block, cap)

    OWN, MATE, NEAR, FAR, ALL = (j, 1), (near, 1), (side[0], 2), (side[1], 2), (0, N_EP)

    def group(ref, p, g):
        return ref[p, pl.ds(*g)].reshape(g[1] * block, ref.shape[-1])

    def put(ref, p, g, value):
        ref[p, pl.ds(*g)] = value.reshape(g[1], block, value.shape[-1])

    def wait_rows(t, p, far):
        wait_bytes(recv_v.at[t, p, pl.ds(0, 1 + far)], disp_recv.at[t, p, far])

    def one_dot(lhs, w_ref, p, which, dims=((1,), (0,))):
        mask = (mask0, mask1)[which]
        return dot(lhs * mask[: lhs.shape[0]], w_ref[2 * p + which], dims)

    def pair_dot(lhs, w_ref, p, *loads):
        terms = []
        for which in HALVES:
            if loads:
                loads[which].wait()
            terms.append(one_dot(lhs, w_ref, p, which))
        return terms[0] + terms[1]

    place = [z, N_TP - 1 - z]
    ahead, behind = [right, left], [left, right]

    cut = block // 16 * 8 + 8
    parts = [pl.ds(0, cut), pl.ds(cut, block - cut)]

    def rows_of(i, part):
        return parts[part] if i == LAST else slice(None)

    def rs_copy(i, h, q, part):
        where = rows_of(i, part)
        return remote(1, part_v.at[i, h, q, where], rs_in.at[i, h, q, where], rs_recv.at[i + part, h, q], tp=ahead[h])

    def rs_start(i, g, part):
        for h in HALVES:
            part_v[i, h, pl.ds(*g)] = part[:, h * half : (h + 1) * half].reshape(g[1], block, half)
        for h in HALVES:
            @pl.when(place[h] == 0)
            def _():
                for first, count in (NEAR, FAR) if g is ALL else (g,):
                    for b in range(count):
                        for n in HALVES if i == LAST else range(1):
                            rs_copy(i, h, first + b, n).start()

    def rs_relay(at, i, far, q, part):
        where = rows_of(i, part)
        for h in HALVES:
            @pl.when(place[h] == at)
            def _():
                rs_copy(i, h, q, part).wait_recv()
                part_v[i, h, q, where] = part_v[i, h, q, where] + rs_in[i, h, q, where]
                rs_copy(i, h, q, part).start()

    def hop_copy(i, h, q, far):
        return remote(2, red_v.at[i, q], slots_v.at[i, h, j], hop_recv.at[i, far], ep=q)

    def turn_copy(i, h, q, far):
        return remote(5, red_v.at[i, q], slots_v.at[i, h, j], hop_recv.at[i, far], tp=behind[h], ep=q)

    def last_turn(h, q, far):
        return remote(7, red_v.at[LAST, q], slots_v.at[LAST, h, j], last_recv.at[0, far, lax.rem(j, 2)], tp=behind[h], ep=q)

    def last_back(h, far, b):
        part = slots_v.at[LAST, h, side[far] + b]
        return remote(8, part, part, last_recv.at[1, far, b], tp=behind[h])

    def last_first(far, b):
        for h in HALVES:
            @pl.when(place[h] == 2)
            def _():
                wait_bytes(slots_v.at[LAST, h, 0], last_recv.at[0, far, b])
                last_back(h, far, b).start()

    def last_second(far, b):
        for h in HALVES:
            @pl.when(place[h] == 1)
            def _():
                last_back(h, far, b).wait_recv()
                last_back(h, far, b).start()

    def last_last(far, b):
        for h in HALVES:
            @pl.when(place[h] == 0)
            def _():
                last_back(h, far, b).wait_recv()

    def rs_final(i, far, q, part):
        where = rows_of(i, part)
        for h in HALVES:
            @pl.when(place[h] == N_TP - 1)
            def _():
                rs_copy(i, h, q, part).wait_recv()
                red_v[i, q, where] = (part_v[i, h, q, where] + rs_in[i, h, q, where]).astype(BF16)
                if i == LAST and part == 0:
                    return
                if i == LAST:
                    last_turn(h, q, far).start()
                else:
                    turn_copy(i, h, q, far).start()
                if far:
                    hop_copy(i, h, q, far).start()
                else:
                    @pl.when(j != q)
                    def _():
                        hop_copy(i, h, q, far).start()

                    @pl.when(j == q)
                    def _():
                        slots_v[i, h, j] = red_v[i, q]

    def hop_wait(i):
        for far in HALVES:
            wait_bytes(slots_v.at[i, 0, pl.ds(0, 1 + far)], hop_recv.at[i, far])

    def hop_wait_end(i):
        @pl.when(at_end)
        def _():
            hop_wait(i)

    def back_copy(i, h, far):
        part = slots_v.at[i, h, pl.ds(side[far], 2)]
        return remote(3, part, part, load_sem.at[2 * i + far], tp=behind[h])

    def back_first(i, far):
        for h in HALVES:
            @pl.when(place[h] == 2)
            def _():
                wait_bytes(slots_v.at[i, h, pl.ds(0, 2)], hop_recv.at[i, far])
                back_copy(i, h, far).start()

    def back_second(i, far):
        for h in HALVES:
            @pl.when(place[h] == 1)
            def _():
                back_copy(i, h, far).wait_recv()
                back_copy(i, h, far).start()

    def back_last(i, far):
        for h in HALVES:
            @pl.when(place[h] == 0)
            def _():
                back_copy(i, h, far).wait_recv()

    def gate_copy(h, at):
        tp = at if h == 0 else N_TP - 1 - at
        return remote(6, gate_rows.at[h], gate_rows.at[h], gate_recv.at[h], tp=tp)

    def gate_root():
        for h in HALVES:
            @pl.when(place[h] == N_TP - 1)
            def _():
                hop_wait(0)
                hop_wait(1)
                y_tok = half_by_token(onehot_slots, slots_v, 0, h)
                part = jnp.sum(gy_v[:, h * half : (h + 1) * half].astype(F32) * y_tok, axis=1, keepdims=True)
                gate_rows[h] = jnp.transpose(jnp.broadcast_to(part, (n_tok, 128)))[:8]
                for at in range(N_TP - 1):
                    gate_copy(h, at).start()

    def wg_copy(k):
        return remote(4, dwg_part, dwg_in.at[k], wg_recv, ep=ep_peer[k])

    def router_back():
        for h in HALVES:
            @pl.when(place[h] != N_TP - 1)
            def _():
                gate_copy(h, 0).wait_recv()
        d_logits = (gate_rows[0, :1] + gate_rows[1, :1]) * router_v[...]
        dwg_part[...] = dot(d_logits.astype(BF16), x_v[...])
        for k in range(3):
            wg_copy(k).start()
        rgrad_v[...] = dot(jnp.transpose(d_logits).astype(BF16), wg_ref[...])

    def forward_act(p, g, *loads):
        a = pair_dot(group(recv_v.at[0], p, g), wi_v, p, *loads)
        put(act_v, p, g, a)
        put(h_v, p, g, (0.5 * a * (1.0 + jnp.tanh(GELU_C * (a + GELU_K * a * a * a)))).astype(BF16))

    def forward_out(p, g, *loads):
        rs_start(p, g, pair_dot(group(h_v, p, g), wo_v, p, *loads))

    NT = ((1,), (1,))

    def backward_act0(p, g):
        put(tmp_v, 0, g, one_dot(group(recv_v.at[1], p, g), wo_v, p, 0, NT))

    def backward_act1(p, g):
        dh = group(tmp_v, 0, g) + one_dot(group(recv_v.at[1], p, g), wo_v, p, 1, NT)
        a = group(act_v, p, g)
        a2 = a * a
        th = jnp.tanh(GELU_C * (a + GELU_K * a2 * a))
        slope = 0.5 * (1.0 + th) + 0.5 * a * (1.0 - th * th) * (GELU_C * (1.0 + 3.0 * GELU_K * a2))
        put(da_v, p, g, (dh * slope).astype(BF16))

    def backward_in0(p, g):
        put(tmp_v, 1, g, one_dot(group(da_v, p, g), wi_v, p, 0, NT))

    def backward_in1(p, g):
        rs_start(2 + p, g, group(tmp_v, 1, g) + one_dot(group(da_v, p, g), wi_v, p, 1, NT))

    def weight_grad(n):
        e = n // 2
        p, mask = e // 2, (mask0, mask1)[e % 2]
        if n % 2 == 0:
            dwo_v[e] = dot(group(h_v, p, ALL) * mask, group(recv_v.at[1], p, ALL), ((0,), (0,)))
        else:
            dwi_v[e] = dot(group(recv_v.at[0], p, ALL) * mask, group(da_v, p, ALL), ((0,), (0,)))

    order = [(0, 0, OWN), (0, 0, MATE), (1, 0, NEAR), (2, 0, NEAR), (0, 1, FAR), (1, 1, FAR), (2, 1, FAR), (3, 0, NEAR), (3, 1, FAR)]
    chunks = [(i, far, g[0] + b, n) for i, far, g in order for b in range(g[1]) for n in (HALVES if i == LAST else range(1))]

    pieces = [(0, 0), (1, 0), (2, 0), (0, 1), (1, 1), (2, 1)]

    def relay(at, k):
        with jax.named_scope(f"relay{at}_{k}"):
            if at == 3:
                back_first(*pieces[k])
            else:
                rs_relay(at, *chunks[k])

    def wait_both(t, p):
        wait_rows(t, p, 0)
        wait_rows(t, p, 1)

    def own_act():
        forward_act(0, OWN, *load_wi[:2])

    def own_out():
        forward_out(0, OWN, *load_wo[:2])

    def start_mate():
        wait_rows(0, 0, 0)
        forward_act(0, MATE)
        forward_out(0, MATE)

    def near_next():
        load_wi[2].wait()
        wait_rows(0, 1, 0)
        forward_act(1, NEAR)

    def near_next_out():
        load_wo[2].wait()
        forward_out(1, NEAR)

    def back_units(p, g, wait):
        def head():
            wait()
            backward_act0(p, g)

        return [head] + [functools.partial(f, p, g) for f in (backward_act1, backward_in0, backward_in1)]

    def far_units(p):
        def head():
            wait_rows(0, p, 1)
            forward_act(p, FAR)

        return [head, functools.partial(forward_out, p, FAR)]

    step("route_x", route_x)
    step("meet", meet)
    start_dispatch(0)
    step("own_act", own_act)
    step("own_out", own_out)
    step("mate", start_mate)
    step("route_dy", route_dy)
    keep_own(1)
    start_dispatch(1)
    step("near1", near_next)
    step("near1_out", near_next_out)

    def timed(ready, lengths, units):
        return [(ready, length, f) for length, f in zip(lengths, units)]

    work = timed(7.0, (0.42, 0.62, 0.42, 0.62), back_units(0, NEAR, lambda: wait_rows(1, 0, 0)))
    work += timed(7.9, (0.62, 0.62), far_units(0)) + timed(11.0, (0.62, 0.62), far_units(1))
    work += timed(13.5, (0.42, 0.6, 0.42, 0.6), back_units(0, FAR, lambda: wait_rows(1, 0, 1)))
    work += timed(16.5, (0.47, 0.65, 0.47, 0.65), back_units(1, ALL, lambda: wait_both(1, 1)))
    work += timed(16.5, (0.61,) * 8, [functools.partial(weight_grad, n) for n in range(8)])
    when = [1.33 * (min(k, 12) + max(k - 12, 0) / 2) for k in range(20)]
    relays = [(start + t, at, k) for start, at in ((7.0, 1), (11.4, 2)) for k, t in enumerate(when)]
    relays = sorted(relays + [(28.4 + 1.31 * k, 3, k) for k in range(3)])
    now, n_work = 7.2, 0
    while relays or work:
        due = relays[0][0] if relays else 1e9
        ready = work[0][0] if work else 1e9
        if work and ready <= now and (now + work[0][1] <= due + 0.15):
            step(f"work{n_work}", work[0][2])
            now += work.pop(0)[1]
            n_work += 1
        elif relays and due <= max(now, ready):
            relay(*relays.pop(0)[1:])
            now = max(now, due) + 0.1
        else:
            now = min(due, max(now, ready)) if ready > now else due

    def turn(i, far):
        step("back1_", back_first, i, far)

    def back(i, far):
        step("back2_", back_second, i, far)

    for k, chunk in enumerate(chunks):
        step(f"final{k}", lambda: rs_final(*chunk))
        if k == 12:
            step("gate_root", gate_root)
    def finish_wg():
        wait_bytes(dwg_in, wg_recv)
        dwg_v[...] = (dwg_part[...] + dwg_in[0]) + (dwg_in[1] + dwg_in[2])

    blocks = [(far, b) for far in HALVES for b in HALVES]
    for n in range(2, 6):
        if n > 2:
            turn(*pieces[n])
        back(*pieces[n - 2])
    step("router_back", router_back)
    back(*pieces[4])
    step("last_first", last_first, *blocks[0])
    step("last_first", last_first, *blocks[1])
    back(*pieces[5])
    step("last_first", last_first, *blocks[2])
    step("last_first", last_first, *blocks[3])
    for far, b in blocks:
        step("last_second", last_second, far, b)
    for piece in pieces:
        step("back3_", back_last, *piece)
    for far, b in blocks:
        step("last_last", last_last, far, b)
    step("hop_", hop_wait_end, 2)
    step("hop_", hop_wait_end, 3)
    step("finish_wg", finish_wg)

    def drain():
        wait_bytes(part_v.at[pl.ds(0, N_EP - 1), 0], sent_sem.at[0])
        wait_bytes(dwg_in, sent_sem.at[4])

        @pl.when(at_end)
        def _():
            wait_bytes(part_v.at[:, 0], sent_sem.at[1])
            wait_bytes(red_v.at[:, pl.ds(0, N_EP - 1)], sent_sem.at[2])
            wait_bytes(red_v.at[pl.ds(0, 3)], sent_sem.at[5])
            wait_bytes(red_v.at[0], sent_sem.at[7])
            wait_bytes(gate_rows.at[pl.ds(0, 3)], sent_sem.at[6])

        @pl.when(jnp.logical_not(at_end))
        def _():
            wait_bytes(part_v, sent_sem.at[1])
            wait_bytes(slots_v.at[pl.ds(0, 3)], sent_sem.at[3])
            wait_bytes(slots_v.at[0], sent_sem.at[8])

    step("drain", drain)


def store_kernel(
    gate_v, back_v, onehot_slots, rgrad_v, dwg_v, dwi_v, dwo_v, out_hbm, dx_hbm, dwg_hbm, dwi_hbm, dwo_hbm, out_v, dx_v, sem
):
    pairs = [(dwi_v.at[e], dwi_hbm.at[e]) for e in range(4)] + [(dwo_v.at[e], dwo_hbm.at[e]) for e in range(4)]
    pairs += [(dwg_v, dwg_hbm), (out_v, out_hbm), (dx_v, dx_hbm)]
    copies = [pltpu.make_async_copy(src, dst, sem.at[n]) for n, (src, dst) in enumerate(pairs)]
    for cp in copies[:-2]:
        cp.start()
    out_v[...] = (gate_v[:, :1] * by_token(onehot_slots, back_v, 0)).astype(BF16)
    copies[-2].start()
    dx_v[...] = (by_token(onehot_slots, back_v, 2) + rgrad_v[...]).astype(BF16)
    copies[-1].start()
    for cp in copies:
        cp.wait()


def solution(mesh):
    row_spec = P(("dp", "ep"), None)

    def local_block(tokens, grad_out, w_router, w_in, w_out, expert_ids):
        n_tok, d_model = tokens.shape
        n_exp = w_router.shape[1]
        n_loc, _, f_loc = w_in.shape
        cap = (6 * n_tok + 5 * n_exp - 1) // (5 * n_exp)
        block, rows, half = 2 * cap, 8 * cap, d_model // 2
        S = jax.ShapeDtypeStruct
        any_spec, vmem_spec = pl.BlockSpec(memory_space=pl.ANY), pl.BlockSpec(memory_space=pltpu.VMEM)
        dma = pltpu.SemaphoreType.DMA
        out_shape = (
            S((n_tok, d_model), BF16), S((n_tok, d_model), BF16), S((n_exp, d_model), F32),
            S((n_loc, d_model, f_loc), F32), S((n_loc, f_loc, d_model), F32),
        )
        handed = (
            S((n_tok, 128), F32), S((4, 2, N_EP, block, half), BF16), S((2 * rows, n_tok), BF16), S((n_tok, d_model), F32),
        ) + out_shape[2:]
        held = tuple(pltpu.VMEM(s.shape, s.dtype) for s in handed)
        scratch = [
            pltpu.VMEM((1, n_tok), jnp.int32), pltpu.VMEM((n_exp, d_model), BF16),
            pltpu.VMEM((n_tok, d_model), BF16), pltpu.VMEM((n_tok, d_model), BF16),
            pltpu.VMEM(w_in.shape, BF16), pltpu.VMEM(w_out.shape, BF16),
            pltpu.VMEM((n_exp, n_tok), F32),
            pltpu.VMEM((2, 2, N_EP, block, d_model), BF16), pltpu.VMEM((2, 2, N_EP, block, d_model), BF16),
            pltpu.VMEM((2, N_EP, block, f_loc), F32), pltpu.VMEM((2, N_EP, block, f_loc), BF16),
            pltpu.VMEM((2, N_EP, block, f_loc), BF16), pltpu.VMEM((2, N_EP, block, d_model), F32),
            pltpu.VMEM((4, 2, N_EP, block, half), F32), pltpu.VMEM((4, 2, N_EP, block, half), F32),
            pltpu.VMEM((4, N_EP, block, half), BF16),
            pltpu.VMEM((n_exp, d_model), F32), pltpu.VMEM((3, n_exp, d_model), F32), pltpu.VMEM((4, 8, n_tok), F32),
            dma((10,)), dma((9,)), dma((2, 2, 2)), dma((5, 2, N_EP)), dma((4, 2)), dma((2, 2, 2)), dma, dma((2,)),
        ]
        results = pl.pallas_call(
            functools.partial(moe_kernel, cap),
            out_shape=held,
            in_specs=[any_spec] * 6,
            out_specs=(vmem_spec,) * 7,
            scratch_shapes=scratch,
            compiler_params=pltpu.CompilerParams(collective_id=0, has_side_effects=True, vmem_limit_bytes=24 * 2**20),
        )(*[
            pltpu.with_memory_space_constraint(r, pltpu.HBM)
            for r in (expert_ids.reshape(1, n_tok), w_router.T, tokens, grad_out, w_in, w_out)
        ])
        out, dx, dwg, dwi, dwo = pl.pallas_call(
            store_kernel,
            out_shape=out_shape,
            in_specs=[vmem_spec] * 7,
            out_specs=(any_spec,) * 5,
            scratch_shapes=[pltpu.VMEM((n_tok, d_model), BF16), pltpu.VMEM((n_tok, d_model), BF16), dma((11,))],
            compiler_params=pltpu.CompilerParams(vmem_limit_bytes=8 * 2**20),
        )(*[pltpu.with_memory_space_constraint(r, pltpu.VMEM) for r in results])
        return out, dx, dwi, dwo, dwg.T

    in_specs = (row_spec, row_spec, P(None, None), P("ep", None, "tp"), P("ep", "tp", None), P(("dp", "ep")))
    out_specs = (row_spec, row_spec, P(("dp", "ep"), None, "tp"), P(("dp", "ep"), "tp", None), P("dp", None))
    return jax.shard_map(local_block, mesh=mesh, in_specs=in_specs, out_specs=out_specs, check_vma=False)
```
